32 devices in a mesh: wide: 8 (over y, x, core), narrow: 4 (over z).
Axes of the slice: x: 2, y: 2, z: 4, core: 2. Of those that a mesh axis runs over, the one named last changes fastest.
Arguments:
- image: bfloat16 [2, 256, 256, 256], P(None, 'wide', 'narrow'), may hold values from -6 to 6
- deapodization: float32 [3, 256], replicated, may hold values from 0.5 to 2
- offsets: int32 [32, 8], P(('wide', 'narrow')), may hold values from 0 to 256
- cross_weight: bfloat16 [32, 8, 1536, 1024], P(('wide', 'narrow')), may hold values from -0.1875 to 0.1875
- x_weight: bfloat16 [32, 8, 1536, 256], P(('wide', 'narrow')), may hold values from -0.375 to 0.375
Outputs:
- samples: float32 [32, 8, 2, 1536], P(('wide', 'narrow'))
The draws below stay inside these ranges and needn't reach their ends.
Inputs may be any that keep to these rules, and one draw needn't show every extreme that they name: `offsets`: each entry is the first row, along the first frequency dimension, of a group's window of 256 rows in one slab.
All inputs are finite; a program needn't handle non-finite values.
Results may differ from the reference program's by a relative error of at most 0.007.
Values may be sent and summed in bfloat16 or wider, within the bound.
A program may use at most 128 MiB of HBM per device.

```python
import math
import jax
import jax.numpy as jnp
from jax import lax

N = 256
G = 512
KZ = 64
BX = 256
SAMP = 1536
CROSS = 1024
GROUPS = 32
N_WIDE = 8
N_NARROW = 4


def plant(array, stream_key, least, high):
    place = [jax.random.randint(jax.random.fold_in(stream_key, axis), (), 0, length) for axis, length in enumerate(array.shape)]
    longest = array.shape.index(max(array.shape))
    beside = place[:longest] + [(place[longest] + 1) % array.shape[longest]] + place[longest + 1:]
    return array.at[tuple(place)].set(least).at[tuple(beside)].set(high)


def steps_of(key, shape, cuts, least, high):
    level = 1.0
    for axis_at, shards_of in cuts:
        heights = jax.random.uniform(jax.random.fold_in(jax.random.fold_in(key, 6), axis_at), (shards_of,), jnp.float32, least / len(cuts), high / len(cuts))
        level = level * jnp.repeat(jnp.exp(heights), shape[axis_at] // shards_of).reshape((-1,) + (1,) * (len(shape) - 1 - axis_at))
    return level


def normal_values(key, dims, width, most, split=(), held_as=jnp.bfloat16):
    result = jax.random.normal(key, dims, jnp.float32) * width
    if len(split) > 0:
        result = steps_of(key, dims, split, -0.22, 0.18) * result
    return jnp.clip(result, min=-most, max=most).astype(held_as)


def setup_inputs(seed: int = 0) -> dict:
    arg_keys = jax.random.split(jax.random.key(seed), 6)
    return {
        "image": normal_values(arg_keys[0], (2, N, N, N), 1.0, 6.0, ((1, 8), (2, 4))),
        "deapodization": jnp.clip(jnp.exp(jax.random.uniform(arg_keys[1], (3, N), jnp.float32, math.log(0.5), math.log(2.0))), 0.5, 2.0),
        "offsets": plant(jax.random.randint(arg_keys[2], (GROUPS, N_WIDE), 0, G - BX + 1), jax.random.fold_in(arg_keys[2], 1), 0, G - BX).astype(jnp.int32),
        "cross_weight": normal_values(arg_keys[3], (GROUPS, N_WIDE, SAMP, CROSS), CROSS ** -0.5, 0.1875, ((0, 32),)),
        "x_weight": normal_values(arg_keys[4], (GROUPS, N_WIDE, SAMP, BX), BX ** -0.5, 0.375, ((0, 32),)),
    }


def dft_tables(out_rows, inputs, grid_size, lowest):
    frequency = jnp.arange(out_rows, dtype=jnp.int32) + lowest
    position = jnp.arange(inputs, dtype=jnp.int32) - inputs // 2
    phases = jnp.mod(frequency[:, None] * position[None, :], grid_size)
    angles = phases.astype(jnp.float32) * (2.0 * math.pi / grid_size)
    factor = 1.0 / math.sqrt(inputs)
    return jnp.stack([jnp.cos(angles) * factor, jnp.sin(angles) * factor]).astype(jnp.bfloat16)

def mix_parts(product):
    return (product[0, 0] + product[1, 1], product[0, 1] - product[1, 0])

def reference(image, deapodization, offsets, cross_weight, x_weight):
    weighted = (image.astype(jnp.float32) * deapodization[0][None, :, None, None] * deapodization[1][None, None, :, None] * deapodization[2][None, None, None, :]).astype(jnp.bfloat16)
    z_table = dft_tables(KZ, N, G, -(KZ // 2)).astype(jnp.float32)
    product = jnp.einsum('tkz,cxyz->tcxyk', z_table, weighted.astype(jnp.float32))
    real_part, imag_part = mix_parts(product)
    band_data = jnp.stack([real_part, imag_part], axis=0).astype(jnp.bfloat16)
    line_table = dft_tables(G, N, G, -(G // 2)).astype(jnp.float32)
    product = jnp.einsum('tqy,cxyk->tcxqk', line_table, band_data.astype(jnp.float32))
    real_part, imag_part = mix_parts(product)
    columns = jnp.stack([real_part, imag_part], axis=0).astype(jnp.bfloat16)
    product = jnp.einsum('tpx,cxqk->tcpqk', line_table, columns.astype(jnp.float32))
    real_part, imag_part = mix_parts(product)
    kspace = jnp.stack([real_part, imag_part], axis=1).astype(jnp.bfloat16)
    span_y = G // N_WIDE
    span_z = KZ // N_NARROW

    def group_samples(group_index):
        narrow_pos = group_index % N_NARROW

        def slab_samples(slab_index):
            start_row = offsets[group_index, slab_index]
            window_rows = lax.dynamic_slice(kspace, (start_row, jnp.int32(0), slab_index * span_y, narrow_pos * span_z), (BX, 2, span_y, span_z)).reshape(BX, 2, span_y * span_z)
            cross_rows = cross_weight[group_index, slab_index].astype(jnp.float32)
            partial_value = jnp.einsum('ms,qcs->cmq', cross_rows, window_rows.astype(jnp.float32))
            window_gain = x_weight[group_index, slab_index].astype(jnp.float32)
            return lax.optimization_barrier(jnp.sum(partial_value * window_gain[None], axis=-1))
        return lax.map(slab_samples, jnp.arange(N_WIDE, dtype=jnp.int32))
    return lax.map(group_samples, jnp.arange(N_WIDE * N_NARROW, dtype=jnp.int32))
```

```python
import functools
import math

import jax
import jax.numpy as jnp
import numpy as np
from jax import lax
from jax.experimental import pallas as pl
from jax.experimental.pallas import tpu as pltpu
from jax.sharding import PartitionSpec as P

G = 512
KZ = 64
BX = 256


def base_tables(out_rows, inputs, grid_size, lowest):
    frequency = np.arange(out_rows, dtype=np.int64) + lowest
    position = np.arange(inputs, dtype=np.int64) - inputs // 2
    phases = np.mod(frequency[:, None] * position[None, :], grid_size)
    angles = phases.astype(np.float64) * (2.0 * math.pi / grid_size)
    factor = 1.0 / math.sqrt(inputs)
    cosine = (np.cos(angles) * factor).astype(np.float32).astype(jnp.bfloat16)
    sine = (np.sin(angles) * factor).astype(np.float32).astype(jnp.bfloat16)
    return cosine, sine


def complex_table(cosine, sine):
    real_rows = np.stack([cosine, sine], axis=1)
    imag_rows = np.stack([-sine, cosine], axis=1)
    return np.stack([real_rows, imag_rows], axis=0)


def sample_kernel(
    sizes, offsets_ref, band_ref, line_ref, row_ref, x_ref, cross_ref, out_ref, wide_ref, slab_ref, window_ref
):
    depth, grid_rows, width, tile = sizes
    step = pl.program_id(0)
    cells = slab_ref.shape[0]

    @pl.when(step == 0)
    def _():
        def one_plane(k, carry):
            parts = [
                band_ref[:, piece, k].reshape(width, band_ref.shape[-1])
                for piece in range(band_ref.shape[1])
            ]
            plane = jnp.concatenate(parts, axis=-1) if len(parts) > 1 else parts[0]
            lines = lax.dot_general(
                line_ref[...], plane, (((1,), (1,)), ((), ())), preferred_element_type=jnp.float32
            )
            for part in range(2):
                for lane in range(0, width, 128):
                    wide_ref[(part * width + lane) // 128, pl.ds(k, grid_rows, stride=depth), :] = lines[
                        part * grid_rows : (part + 1) * grid_rows, lane : lane + 128
                    ]
            return carry

        for k in range(depth):
            one_plane(k, 0)

    here = pl.ds(pl.multiple_of(step * cells, cells), cells)
    start = offsets_ref[0, step]
    for block in range(2 * width // 128):
        lanes = slice(block * 128, (block + 1) * 128)
        slab_ref[:, lanes] = wide_ref[block, here, :].astype(jnp.bfloat16)
        window_ref[:, lanes] = row_ref[block, pl.ds(start, BX), :].astype(jnp.bfloat16)
    for first in range(0, cross_ref.shape[1], tile):
        rows = slice(first, first + tile)
        partial = jnp.dot(cross_ref[0, rows], slab_ref[...], preferred_element_type=jnp.float32)
        gain = jnp.dot(x_ref[0, rows], window_ref[...], preferred_element_type=jnp.float32)
        part_re, part_im = partial[:, :width], partial[:, width:]
        gain_cos, gain_sin = gain[:, :width], gain[:, width:]
        for part, value in enumerate(
            (gain_cos * part_re + gain_sin * part_im, gain_cos * part_im - gain_sin * part_re)
        ):
            folded = value[:, :128]
            for lane in range(128, width, 128):
                folded = folded + value[:, lane : lane + 128]
            out_ref[0, part : part + 1, rows] = jnp.sum(folded.T, axis=0, keepdims=True)


def gather_kernel(
    wide, narrow, band_ref, out_ref, own_sem, swap_send, swap_recv, chip_send, chip_recv, core_send, core_recv
):
    w = lax.axis_index("wide")
    n = lax.axis_index("narrow")
    sibling = w + 1 - 2 * lax.rem(w, 2)
    chips = wide // 2
    barrier = pltpu.get_barrier_semaphore()
    targets = [(w, lax.rem(n + j, narrow)) for j in range(1, narrow)]
    targets += [(lax.rem(w + 2 * j, wide), n) for j in range(1, chips)] + [(sibling, n)]
    for target in targets:
        pl.semaphore_signal(
            barrier, inc=1, device_id=target, device_id_type=pl.DeviceIdType.MESH
        )
    pl.semaphore_wait(barrier, len(targets))

    def remote(source, place, send, receive, target):
        return pltpu.make_async_remote_copy(
            src_ref=source,
            dst_ref=place,
            send_sem=send,
            recv_sem=receive,
            device_id=target,
            device_id_type=pl.DeviceIdType.MESH,
        )

    swaps = []
    for j in range(1, narrow):
        peer = lax.rem(n + j, narrow)
        swap = remote(
            band_ref.at[peer], out_ref.at[w, n], swap_send.at[j - 1], swap_recv.at[j - 1], (w, peer)
        )
        swap.start()
        swaps.append(swap)
    own = pltpu.make_async_copy(band_ref.at[n], out_ref.at[w, n], own_sem)
    own.start()
    own.wait()
    for swap in swaps:
        swap.wait()
    mine = out_ref.at[w]
    hops = []
    for j in range(1, chips):
        peer = lax.rem(w + 2 * j, wide)
        hop = remote(mine, mine, chip_send.at[j - 1], chip_recv.at[j - 1], (peer, n))
        hop.start()
        hops.append(hop)
    passes = [remote(mine, mine, core_send.at[0], core_recv.at[0], (sibling, n))]
    passes[0].start()
    for j in range(1, chips):
        hops[j - 1].wait_recv()
        block = out_ref.at[lax.rem(w + wide - 2 * j, wide)]
        forward = remote(block, block, core_send.at[j], core_recv.at[j], (sibling, n))
        forward.start()
        passes.append(forward)
    for hop in hops:
        hop.wait_send()
    for forward in passes:
        forward.wait()


def per_device(image, deapodization, offsets, cross_weight, x_weight):
    wide_count = lax.axis_size("wide")
    narrow_count = lax.axis_size("narrow")
    wide_index = lax.axis_index("wide")
    narrow_index = lax.axis_index("narrow")
    block_x = image.shape[1]
    block_y = image.shape[2]
    width = image.shape[3]
    depth = KZ // narrow_count
    samples, cells = cross_weight.shape[2], cross_weight.shape[3]
    scale_x = lax.dynamic_slice_in_dim(deapodization[0], wide_index * block_x, block_x)
    scale_y = lax.dynamic_slice_in_dim(deapodization[1], narrow_index * block_y, block_y)
    weighted = (
        image.astype(jnp.float32)
        * scale_x[None, :, None, None]
        * scale_y[None, None, :, None]
        * deapodization[2][None, None, None, :]
    ).astype(jnp.bfloat16)
    z_table = complex_table(*base_tables(KZ, width, G, -(KZ // 2)))
    band = jnp.einsum(
        "okcz,cxyz->kxoy", jnp.asarray(z_table), weighted, preferred_element_type=jnp.float32
    ).astype(jnp.bfloat16)
    band = band.reshape(KZ, block_x, 2 * block_y)
    band = band.reshape(narrow_count, depth, block_x, 2 * block_y)
    chips = wide_count // 2
    band = pl.pallas_call(
        functools.partial(gather_kernel, wide_count, narrow_count),
        out_shape=jax.ShapeDtypeStruct((wide_count,) + band.shape, band.dtype),
        in_specs=[pl.BlockSpec(memory_space=pltpu.VMEM)],
        out_specs=pl.BlockSpec(memory_space=pltpu.VMEM),
        scratch_shapes=[
            pltpu.SemaphoreType.DMA,
            pltpu.SemaphoreType.DMA((narrow_count - 1,)),
            pltpu.SemaphoreType.DMA((narrow_count - 1,)),
            pltpu.SemaphoreType.DMA((chips - 1,)),
            pltpu.SemaphoreType.DMA((chips - 1,)),
            pltpu.SemaphoreType.DMA((chips,)),
            pltpu.SemaphoreType.DMA((chips,)),
        ],
        compiler_params=pltpu.CompilerParams(collective_id=0, has_side_effects=True),
    )(band)
    if (2 * block_y) % 128:
        band = band.transpose(0, 2, 3, 1, 4).reshape(wide_count, 1, depth, block_x, 2 * width)

    cosine, sine = base_tables(G, width, G, -(G // 2))
    line_table = complex_table(cosine, sine).reshape(2 * G, 2, narrow_count, block_y)
    line_table = line_table.transpose(0, 2, 1, 3).reshape(2 * G, 2 * width)
    row_table = np.concatenate([cosine, sine], axis=1).astype(np.float32)
    row_table = row_table.reshape(G, 2 * width // 128, 128).transpose(1, 0, 2)

    tile = 512 if samples % 512 == 0 else samples
    kernel = functools.partial(sample_kernel, (depth, G, width, tile))
    out = pl.pallas_call(
        kernel,
        grid=(wide_count,),
        out_shape=jax.ShapeDtypeStruct((wide_count, 2, samples), jnp.float32),
        in_specs=[
            pl.BlockSpec(memory_space=pltpu.SMEM),
            pl.BlockSpec(band.shape, lambda s: (0, 0, 0, 0, 0)),
            pl.BlockSpec(line_table.shape, lambda s: (0, 0)),
            pl.BlockSpec(row_table.shape, lambda s: (0, 0, 0)),
            pl.BlockSpec((1, samples, BX), lambda s: (s, 0, 0)),
            pl.BlockSpec((1, samples, cells), lambda s: (s, 0, 0)),
        ],
        out_specs=pl.BlockSpec((1, 2, samples), lambda s: (s, 0, 0)),
        scratch_shapes=[
            pltpu.VMEM((2 * width // 128, G * depth, 128), jnp.float32),
            pltpu.VMEM((cells, 2 * width), jnp.bfloat16),
            pltpu.VMEM((BX, 2 * width), jnp.bfloat16),
        ],
        compiler_params=pltpu.CompilerParams(vmem_limit_bytes=60 * 1024 * 1024),
        cost_estimate=pl.CostEstimate(
            flops=2 * wide_count * samples * 2 * width * (cells + BX) + 8 * G * width * width * depth,
            bytes_accessed=2 * wide_count * samples * (cells + BX),
            transcendentals=0,
        ),
    )(offsets, band, jnp.asarray(line_table), jnp.asarray(row_table), x_weight[0], cross_weight[0])
    return out[None]


def flip(index, bits):
    low = lax.rem(index + bits, 2)
    high = lax.rem(lax.div(index, 2) + lax.div(bits, 2), 2)
    return low + 2 * high


def fused_kernel(
    sizes, image_hbm, deap_smem, deap_ref, offsets_ref, z_hbm, line_hbm, row_hbm, x_hbm, cross_hbm, out_ref,
    image_ref, scale_ref, spread_ref, send_ref, grid_ref, z_ref, line_ref, row_ref, x_ref, window_ref, gain_ref,
    cross_ref, wide_ref, slab_a, slab_b,
    image_sem, table_sem, x_sem, cross_sem,
    swap_send, swap_recv, own_send, near_recv, relay_send, relay_recv, pass_send, pass_recv,
):
    depth, grid_rows, tile = sizes
    w = lax.axis_index("wide")
    n = lax.axis_index("narrow")
    rounds, narrow, wide, _, strip, lanes = grid_ref.shape
    slots = x_ref.shape[0]
    block_y, width = scale_ref.shape
    slabs, samples, cells = cross_ref.shape
    pitch = depth + 1
    half = wide * strip
    span = cells // depth

    core = lax.rem(w, 2)
    across = w + 2 - 4 * lax.rem(lax.div(w, 2), 2)
    along = w + 4 - 8 * lax.rem(lax.div(w, 4), 2)
    first = across + core * (along - across)
    second = along + core * (across - along)
    corner = across + along - w
    sibling = w + 1 - 2 * core
    held = (w, first, second, corner)
    sib_across = across + 1 - 2 * core
    sib_along = along + 1 - 2 * core
    sib_first = sib_along + core * (sib_across - sib_along)
    sib_second = sib_across + core * (sib_along - sib_across)
    theirs = (sibling, sib_first, sib_second, corner + 1 - 2 * core)

    def remote(source, place, send, receive, target):
        return pltpu.make_async_remote_copy(
            src_ref=source, dst_ref=place, send_sem=send, recv_sem=receive,
            device_id=target, device_id_type=pl.DeviceIdType.MESH,
        )

    image_loads = [
        pltpu.make_async_copy(
            image_hbm.at[:, r * strip : (r + 1) * strip],
            image_ref.at[:, r * strip : (r + 1) * strip],
            image_sem.at[r],
        )
        for r in range(rounds)
    ]
    table_loads = [
        pltpu.make_async_copy(source, place, table_sem.at[i])
        for i, (source, place) in enumerate(((z_hbm, z_ref), (row_hbm, row_ref), (line_hbm, line_ref)))
    ]

    def x_load(s):
        return pltpu.make_async_copy(x_hbm.at[s], x_ref.at[s % slots], x_sem.at[s % slots])

    def cross_load(s):
        return pltpu.make_async_copy(cross_hbm.at[s], cross_ref.at[s], cross_sem.at[s])

    image_loads[0].start()
    table_loads[0].start()
    image_loads[1].start()
    barrier = pltpu.get_barrier_semaphore()
    peers = [(w, flip(n, j)) for j in range(1, narrow)] + [(first, n), (second, n), (sibling, n)]
    for peer in peers:
        pl.semaphore_signal(barrier, inc=1, device_id=peer, device_id_type=pl.DeviceIdType.MESH)

    last = deap_ref[2:3, :]
    for y in range(block_y):
        scale_ref[y : y + 1, :] = last * deap_smem[1, n * block_y + y]

    def band(r):
        low = lax.broadcasted_iota(jnp.int32, (narrow * depth, lanes), 1) < block_y
        group = width // block_y
        for at in range(0, strip, group):
            halves = []
            for c in range(2):
                pieces = []
                for x in range(at, at + group):
                    gain = scale_ref[...] * deap_smem[0, w * rounds * strip + r * strip + x]
                    pieces.append((image_ref[c, r * strip + x].astype(jnp.float32) * gain).astype(jnp.bfloat16))
                halves.append(jnp.concatenate(pieces, axis=0))
            both = jnp.concatenate(halves, axis=1)
            value = lax.dot_general(z_ref[...], both, (((1,), (1,)), ((), ())), preferred_element_type=jnp.float32)
            real, imag = value[: narrow * depth], value[narrow * depth :]
            for pair in range(group // 2):
                here = slice(pair * lanes, (pair + 1) * lanes)
                even = jnp.where(low, real[:, here], pltpu.roll(imag[:, here], block_y, 1))
                odd = jnp.where(low, pltpu.roll(real[:, here], block_y, 1), imag[:, here])
                spread_ref[pl.ds(at + 2 * pair, narrow * depth, stride=pitch), :] = even
                spread_ref[pl.ds(at + 2 * pair + 1, narrow * depth, stride=pitch), :] = odd
        for k in range(narrow * depth):
            send_ref[r, k // depth, k % depth] = spread_ref[k * pitch : k * pitch + strip, :].astype(jnp.bfloat16)
        grid_ref[r, n, w] = send_ref[r, n]

    def swap(r, j):
        peer = flip(n, j)
        return remote(
            send_ref.at[r, peer], grid_ref.at[r, n, w], swap_send.at[r, j], swap_recv.at[r, j], (w, peer)
        )

    def place(r, j, column):
        return grid_ref.at[r, flip(n, j), column]

    def own_copies(r, j):
        mine = place(r, j, w)
        return [
            remote(mine, mine, own_send.at[r, j, 0], near_recv.at[r, j, 0], (first, n)),
            remote(mine, mine, own_send.at[r, j, 1], near_recv.at[r, j, 1], (second, n)),
            pass_copy(r, j, 0),
        ]

    def relay_copy(r, j):
        block = place(r, j, first)
        return remote(block, block, relay_send.at[r, j], relay_recv.at[r, j], (second, n))

    def pass_copy(r, j, kind):
        block = place(r, j, held[kind])
        return remote(block, block, pass_send.at[r, j, kind], pass_recv.at[r, j, kind], (sibling, n))

    def arrived(r, j, column, send, receive):
        block = place(r, j, column)
        remote(block, block, send, receive, (sibling, n)).wait_recv()

    def own(r, j):
        if j > 0:
            block = grid_ref.at[r, flip(n, j), w]
            remote(block, block, swap_send.at[r, j], swap_recv.at[r, j], (w, flip(n, j))).wait_recv()
        for copy in own_copies(r, j):
            copy.start()

    def relay(r, j):
        arrived(r, j, first, own_send.at[r, j, 0], near_recv.at[r, j, 0])
        relay_copy(r, j).start()
        pass_copy(r, j, 1).start()

    def near(r, j):
        arrived(r, j, second, own_send.at[r, j, 1], near_recv.at[r, j, 1])
        pass_copy(r, j, 2).start()

    def far(r, j):
        arrived(r, j, corner, relay_send.at[r, j], relay_recv.at[r, j])
        pass_copy(r, j, 3).start()

    def settle(r):
        for j in range(narrow):
            for kind in range(4):
                arrived(r, j, theirs[kind], pass_send.at[r, j, kind], pass_recv.at[r, j, kind])

    def gains(s):
        x_load(s).wait()
        start = offsets_ref[0, s]
        for block in range(row_ref.shape[0]):
            window_ref[:, block * 128 : (block + 1) * 128] = row_ref[block, pl.ds(start, BX), :].astype(jnp.bfloat16)
        for at in range(0, samples, tile):
            rows = slice(at, at + tile)
            gain_ref[s, rows] = jnp.dot(
                x_ref[s % slots, rows], window_ref[...], preferred_element_type=jnp.float32
            ).astype(jnp.bfloat16)
        if s + slots < slabs:
            x_load(s + slots).start()

    def lines(r, k):
        planes = [
            jnp.concatenate([grid_ref[r, source, :, k + i].reshape(half, lanes) for i in range(2)], axis=0)
            for source in range(narrow)
        ]
        plane = jnp.concatenate(planes, axis=1)
        value = lax.dot_general(
            line_ref[...], plane, (((1,), (1,)), ((), ())), preferred_element_type=jnp.float32
        )
        for part in range(2):
            for i in range(2):
                wide_ref[part, pl.ds(k + i, grid_rows, stride=pitch), :] = value[
                    part * grid_rows : (part + 1) * grid_rows, i * half : (i + 1) * half
                ]

    def gather(s, slab_ref):
        base = s * span * pitch
        for part in range(2):
            for y in range(span):
                slab_ref[y * depth : (y + 1) * depth, part * half : (part + 1) * half] = wide_ref[
                    part, pl.ds(base + y * pitch, depth), :
                ].astype(jnp.bfloat16)

    def contract(r, s, slab_ref):
        for at in range(0, samples, tile):
            rows = slice(at, at + tile)
            value = jnp.dot(cross_ref[s, rows], slab_ref[...], preferred_element_type=jnp.float32)
            real, imag = value[:, :half], value[:, half:]
            gain = gain_ref[s, rows, 2 * r * half : 2 * (r + 1) * half].astype(jnp.float32)
            cosine, sine = gain[:, :half], gain[:, half:]
            for part, product in enumerate((cosine * real + sine * imag, cosine * imag - sine * real)):
                total = jnp.sum(product.T, axis=0, keepdims=True)
                if r > 0:
                    total = total + out_ref[s, part : part + 1, rows]
                out_ref[s, part : part + 1, rows] = total

    for copy in table_loads[1:]:
        copy.start()
    for s in range(slots):
        x_load(s).start()
    table_loads[0].wait()
    image_loads[0].wait()
    band(0)
    for s in range(slabs):
        cross_load(s).start()
    pl.semaphore_wait(barrier, len(peers))
    for j in range(1, narrow):
        swap(0, j).start()
    own(0, 0)
    image_loads[1].wait()
    band(1)
    for j in range(1, narrow):
        swap(1, j).start()
    table_loads[1].wait()
    table_loads[2].wait()
    for s in range(4):
        gains(s)
    relay(0, 0)
    own(0, 1)
    for s in range(4, 6):
        gains(s)
    near(0, 0)
    far(0, 0)
    for s in range(6, slabs):
        gains(s)
    relay(0, 1)
    own(0, 2)
    near(0, 1)
    own(0, 3)
    relay(0, 2)
    far(0, 1)
    own(1, 0)
    near(0, 2)
    relay(0, 3)
    far(0, 2)
    near(0, 3)
    own(1, 1)
    far(0, 3)
    relay(1, 0)
    settle(0)

    events = {
        1: [(near, 0), (own, 2)],
        3: [(far, 0), (relay, 1)],
        5: [(near, 1), (own, 3)],
        7: [(far, 1), (relay, 2)],
    }
    for pair in range(depth // 2):
        lines(0, 2 * pair)
        for event, j in events.get(pair, []):
            event(1, j)
    for s in range(slabs):
        cross_load(s).wait()

    gather(0, slab_a)

    def steps(r, i):
        gather(2 * i + 1, slab_b)
        contract(r, 2 * i, slab_a)
        gather(lax.rem(2 * i + 2, slabs), slab_a)
        contract(r, 2 * i + 1, slab_b)

    def early(i, carry):
        steps(0, i)
        return carry

    def late(i, carry):
        steps(1, i)
        return carry

    lax.fori_loop(0, 1, early, 0)
    near(1, 2)
    relay(1, 3)
    lax.fori_loop(1, 2, early, 0)
    far(1, 2)
    near(1, 3)
    lax.fori_loop(2, 3, early, 0)
    far(1, 3)
    lax.fori_loop(3, slabs // 2, early, 0)
    settle(1)
    for pair in range(depth // 2):
        lines(1, 2 * pair)
    gather(0, slab_a)
    lax.fori_loop(0, slabs // 2, late, 0)

    for r in range(rounds):
        for j in range(narrow):
            if j > 0:
                swap(r, j).wait_send()
            for copy in own_copies(r, j):
                copy.wait_send()
            relay_copy(r, j).wait_send()
            for kind in range(1, 4):
                pass_copy(r, j, kind).wait_send()


def fused_device(image, deapodization, offsets, cross_weight, x_weight):
    wide = lax.axis_size("wide")
    narrow = lax.axis_size("narrow")
    block_x, block_y, width = image.shape[1:]
    depth = KZ // narrow
    slabs, samples, cells = cross_weight.shape[1:]
    rounds = 2
    strip = block_x // rounds
    lanes = 2 * block_y
    slots = 4
    z_table = complex_table(*base_tables(KZ, width, G, -(KZ // 2))).reshape(2 * KZ, 2 * width)
    cosine, sine = base_tables(G, width, G, -(G // 2))
    line_table = complex_table(cosine, sine).reshape(2 * G, 2, narrow, block_y)
    line_table = line_table.transpose(0, 2, 1, 3).reshape(2 * G, 2 * width)
    row_table = np.stack([cosine, sine], axis=0).astype(np.float32).reshape(2, G, wide, rounds, strip)
    row_table = row_table.transpose(3, 0, 1, 2, 4).reshape(2 * rounds, G, wide * strip)
    hbm = pl.BlockSpec(memory_space=pl.ANY)
    vmem = pl.BlockSpec(memory_space=pltpu.VMEM)
    smem = pl.BlockSpec(memory_space=pltpu.SMEM)
    dma = pltpu.SemaphoreType.DMA
    half = wide * strip
    out = pl.pallas_call(
        functools.partial(fused_kernel, (depth, G, 512 if samples % 512 == 0 else samples)),
        out_shape=jax.ShapeDtypeStruct((slabs, 2, samples), jnp.float32),
        in_specs=[hbm, smem, vmem, smem, hbm, hbm, hbm, hbm, hbm],
        out_specs=vmem,
        scratch_shapes=[
            pltpu.VMEM(image.shape, jnp.bfloat16),
            pltpu.VMEM((block_y, width), jnp.float32),
            pltpu.VMEM((KZ * (depth + 1), lanes), jnp.float32),
            pltpu.VMEM((rounds, narrow, depth, strip, lanes), jnp.bfloat16),
            pltpu.VMEM((rounds, narrow, wide, depth, strip, lanes), jnp.bfloat16),
            pltpu.VMEM(z_table.shape, jnp.bfloat16),
            pltpu.VMEM(line_table.shape, jnp.bfloat16),
            pltpu.VMEM(row_table.shape, jnp.float32),
            pltpu.VMEM((slots, samples, BX), jnp.bfloat16),
            pltpu.VMEM((BX, 2 * width), jnp.bfloat16),
            pltpu.VMEM((slabs, samples, 2 * width), jnp.bfloat16),
            pltpu.VMEM((slabs, samples, cells), jnp.bfloat16),
            pltpu.VMEM((2, G * (depth + 1), half), jnp.float32),
            pltpu.VMEM((cells, 2 * half), jnp.bfloat16),
            pltpu.VMEM((cells, 2 * half), jnp.bfloat16),
            dma((rounds,)),
            dma((3,)),
            dma((slots,)),
            dma((slabs,)),
            dma((rounds, narrow)),
            dma((rounds, narrow)),
            dma((rounds, narrow, 2)),
            dma((rounds, narrow, 2)),
            dma((rounds, narrow)),
            dma((rounds, narrow)),
            dma((rounds, narrow, 4)),
            dma((rounds, narrow, 4)),
        ],
        compiler_params=pltpu.CompilerParams(
            vmem_limit_bytes=67043328, collective_id=1, has_side_effects=True
        ),
    )(
        image, deapodization, deapodization, offsets, jnp.asarray(z_table), jnp.asarray(line_table),
        jnp.asarray(row_table), x_weight[0], cross_weight[0],
    )
    return out[None]


def solution(mesh):
    square = mesh.shape["wide"] == 8 and mesh.shape["narrow"] == 4
    return jax.shard_map(
        fused_device if square else per_device,
        mesh=mesh,
        in_specs=(
            P(None, "wide", "narrow", None),
            P(),
            P(("wide", "narrow"), None),
            P(("wide", "narrow"), None, None, None),
            P(("wide", "narrow"), None, None, None),
        ),
        out_specs=P(("wide", "narrow"), None, None, None),
        check_vma=False,
    )
```

```python
import functools
import math

import jax
import jax.numpy as jnp
import numpy as np
from jax import lax
from jax.experimental import pallas as pl
from jax.experimental.pallas import tpu as pltpu
from jax.sharding import PartitionSpec as P

G = 512
KZ = 64
BX = 256
TILE = 128


def base_tables(out_rows, inputs, grid_size, lowest):
    frequency = np.arange(out_rows, dtype=np.int64) + lowest
    position = np.arange(inputs, dtype=np.int64) - inputs // 2
    phases = np.mod(frequency[:, None] * position[None, :], grid_size)
    angles = phases.astype(np.float64) * (2.0 * math.pi / grid_size)
    factor = 1.0 / math.sqrt(inputs)
    cosine = (np.cos(angles) * factor).astype(np.float32).astype(jnp.bfloat16)
    sine = (np.sin(angles) * factor).astype(np.float32).astype(jnp.bfloat16)
    return cosine, sine


def complex_table(cosine, sine):
    real_rows = np.stack([cosine, sine], axis=1)
    imag_rows = np.stack([-sine, cosine], axis=1)
    return np.stack([real_rows, imag_rows], axis=0)


def sample_kernel(
    sizes, offsets_ref, band_ref, line_ref, row_ref, x_ref, cross_ref, out_ref, wide_ref, slab_ref, window_ref
):
    depth, grid_rows, width, tile = sizes
    step = pl.program_id(0)
    cells = slab_ref.shape[0]

    @pl.when(step == 0)
    def _():
        def one_plane(k, carry):
            parts = [
                band_ref[:, piece, k].reshape(width, band_ref.shape[-1])
                for piece in range(band_ref.shape[1])
            ]
            plane = jnp.concatenate(parts, axis=-1) if len(parts) > 1 else parts[0]
            lines = lax.dot_general(
                line_ref[...], plane, (((1,), (1,)), ((), ())), preferred_element_type=jnp.float32
            )
            for part in range(2):
                for lane in range(0, width, 128):
                    wide_ref[(part * width + lane) // 128, pl.ds(k, grid_rows, stride=depth), :] = lines[
                        part * grid_rows : (part + 1) * grid_rows, lane : lane + 128
                    ]
            return carry

        for k in range(depth):
            one_plane(k, 0)

    here = pl.ds(pl.multiple_of(step * cells, cells), cells)
    start = offsets_ref[0, step]
    for block in range(2 * width // 128):
        lanes = slice(block * 128, (block + 1) * 128)
        slab_ref[:, lanes] = wide_ref[block, here, :].astype(jnp.bfloat16)
        window_ref[:, lanes] = row_ref[block, pl.ds(start, BX), :].astype(jnp.bfloat16)
    for first in range(0, cross_ref.shape[1], tile):
        rows = slice(first, first + tile)
        partial = jnp.dot(cross_ref[0, rows], slab_ref[...], preferred_element_type=jnp.float32)
        gain = jnp.dot(x_ref[0, rows], window_ref[...], preferred_element_type=jnp.float32)
        part_re, part_im = partial[:, :width], partial[:, width:]
        gain_cos, gain_sin = gain[:, :width], gain[:, width:]
        for part, value in enumerate(
            (gain_cos * part_re + gain_sin * part_im, gain_cos * part_im - gain_sin * part_re)
        ):
            folded = value[:, :128]
            for lane in range(128, width, 128):
                folded = folded + value[:, lane : lane + 128]
            out_ref[0, part : part + 1, rows] = jnp.sum(folded.T, axis=0, keepdims=True)


def gather_kernel(
    wide, narrow, band_ref, out_ref, own_sem, swap_send, swap_recv, chip_send, chip_recv, core_send, core_recv
):
    w = lax.axis_index("wide")
    n = lax.axis_index("narrow")
    sibling = w + 1 - 2 * lax.rem(w, 2)
    chips = wide // 2
    barrier = pltpu.get_barrier_semaphore()
    targets = [(w, lax.rem(n + j, narrow)) for j in range(1, narrow)]
    targets += [(lax.rem(w + 2 * j, wide), n) for j in range(1, chips)] + [(sibling, n)]
    for target in targets:
        pl.semaphore_signal(
            barrier, inc=1, device_id=target, device_id_type=pl.DeviceIdType.MESH
        )
    pl.semaphore_wait(barrier, len(targets))

    def remote(source, place, send, receive, target):
        return pltpu.make_async_remote_copy(
            src_ref=source,
            dst_ref=place,
            send_sem=send,
            recv_sem=receive,
            device_id=target,
            device_id_type=pl.DeviceIdType.MESH,
        )

    swaps = []
    for j in range(1, narrow):
        peer = lax.rem(n + j, narrow)
        swap = remote(
            band_ref.at[peer], out_ref.at[w, n], swap_send.at[j - 1], swap_recv.at[j - 1], (w, peer)
        )
        swap.start()
        swaps.append(swap)
    own = pltpu.make_async_copy(band_ref.at[n], out_ref.at[w, n], own_sem)
    own.start()
    own.wait()
    for swap in swaps:
        swap.wait()
    mine = out_ref.at[w]
    hops = []
    for j in range(1, chips):
        peer = lax.rem(w + 2 * j, wide)
        hop = remote(mine, mine, chip_send.at[j - 1], chip_recv.at[j - 1], (peer, n))
        hop.start()
        hops.append(hop)
    passes = [remote(mine, mine, core_send.at[0], core_recv.at[0], (sibling, n))]
    passes[0].start()
    for j in range(1, chips):
        hops[j - 1].wait_recv()
        block = out_ref.at[lax.rem(w + wide - 2 * j, wide)]
        forward = remote(block, block, core_send.at[j], core_recv.at[j], (sibling, n))
        forward.start()
        passes.append(forward)
    for hop in hops:
        hop.wait_send()
    for forward in passes:
        forward.wait()


def per_device(image, deapodization, offsets, cross_weight, x_weight):
    wide_count = lax.axis_size("wide")
    narrow_count = lax.axis_size("narrow")
    wide_index = lax.axis_index("wide")
    narrow_index = lax.axis_index("narrow")
    block_x = image.shape[1]
    block_y = image.shape[2]
    width = image.shape[3]
    depth = KZ // narrow_count
    samples, cells = cross_weight.shape[2], cross_weight.shape[3]
    scale_x = lax.dynamic_slice_in_dim(deapodization[0], wide_index * block_x, block_x)
    scale_y = lax.dynamic_slice_in_dim(deapodization[1], narrow_index * block_y, block_y)
    weighted = (
        image.astype(jnp.float32)
        * scale_x[None, :, None, None]
        * scale_y[None, None, :, None]
        * deapodization[2][None, None, None, :]
    ).astype(jnp.bfloat16)
    z_table = complex_table(*base_tables(KZ, width, G, -(KZ // 2)))
    band = jnp.einsum(
        "okcz,cxyz->kxoy", jnp.asarray(z_table), weighted, preferred_element_type=jnp.float32
    ).astype(jnp.bfloat16)
    band = band.reshape(KZ, block_x, 2 * block_y)
    band = band.reshape(narrow_count, depth, block_x, 2 * block_y)
    chips = wide_count // 2
    band = pl.pallas_call(
        functools.partial(gather_kernel, wide_count, narrow_count),
        out_shape=jax.ShapeDtypeStruct((wide_count,) + band.shape, band.dtype),
        in_specs=[pl.BlockSpec(memory_space=pltpu.VMEM)],
        out_specs=pl.BlockSpec(memory_space=pltpu.VMEM),
        scratch_shapes=[
            pltpu.SemaphoreType.DMA,
            pltpu.SemaphoreType.DMA((narrow_count - 1,)),
            pltpu.SemaphoreType.DMA((narrow_count - 1,)),
            pltpu.SemaphoreType.DMA((chips - 1,)),
            pltpu.SemaphoreType.DMA((chips - 1,)),
            pltpu.SemaphoreType.DMA((chips,)),
            pltpu.SemaphoreType.DMA((chips,)),
        ],
        compiler_params=pltpu.CompilerParams(collective_id=0, has_side_effects=True),
    )(band)
    if (2 * block_y) % 128:
        band = band.transpose(0, 2, 3, 1, 4).reshape(wide_count, 1, depth, block_x, 2 * width)

    cosine, sine = base_tables(G, width, G, -(G // 2))
    line_table = complex_table(cosine, sine).reshape(2 * G, 2, narrow_count, block_y)
    line_table = line_table.transpose(0, 2, 1, 3).reshape(2 * G, 2 * width)
    row_table = np.concatenate([cosine, sine], axis=1).astype(np.float32)
    row_table = row_table.reshape(G, 2 * width // 128, 128).transpose(1, 0, 2)

    tile = 512 if samples % 512 == 0 else samples
    kernel = functools.partial(sample_kernel, (depth, G, width, tile))
    out = pl.pallas_call(
        kernel,
        grid=(wide_count,),
        out_shape=jax.ShapeDtypeStruct((wide_count, 2, samples), jnp.float32),
        in_specs=[
            pl.BlockSpec(memory_space=pltpu.SMEM),
            pl.BlockSpec(band.shape, lambda s: (0, 0, 0, 0, 0)),
            pl.BlockSpec(line_table.shape, lambda s: (0, 0)),
            pl.BlockSpec(row_table.shape, lambda s: (0, 0, 0)),
            pl.BlockSpec((1, samples, BX), lambda s: (s, 0, 0)),
            pl.BlockSpec((1, samples, cells), lambda s: (s, 0, 0)),
        ],
        out_specs=pl.BlockSpec((1, 2, samples), lambda s: (s, 0, 0)),
        scratch_shapes=[
            pltpu.VMEM((2 * width // 128, G * depth, 128), jnp.float32),
            pltpu.VMEM((cells, 2 * width), jnp.bfloat16),
            pltpu.VMEM((BX, 2 * width), jnp.bfloat16),
        ],
        compiler_params=pltpu.CompilerParams(vmem_limit_bytes=60 * 1024 * 1024),
        cost_estimate=pl.CostEstimate(
            flops=2 * wide_count * samples * 2 * width * (cells + BX) + 8 * G * width * width * depth,
            bytes_accessed=2 * wide_count * samples * (cells + BX),
            transcendentals=0,
        ),
    )(offsets, band, jnp.asarray(line_table), jnp.asarray(row_table), x_weight[0], cross_weight[0])
    return out[None]


def flip(index, bits):
    low = lax.rem(index + bits, 2)
    high = lax.rem(lax.div(index, 2) + lax.div(bits, 2), 2)
    return low + 2 * high


def fused_kernel(
    sizes, image_hbm, deap_hbm, offsets_hbm, z_hbm, line_hbm, row_hbm, x_hbm, cross_hbm, out_ref,
    deap_smem, deap_ref, offsets_ref, image_ref, scale_ref, perm_ref, spread_ref, send_ref, grid_ref, z_ref, line_ref, packed_ref, row_ref, x_ref, window_a, window_b, gain_ref,
    cross_ref, wide_ref, slab_a, slab_b,
    small_sem, image_sem, table_sem, x_sem, cross_sem,
    swap_send, swap_recv, own_send, near_recv, relay_send, relay_recv, pass_send, pass_recv,
):
    depth, grid_rows, tile = sizes
    w = lax.axis_index("wide")
    n = lax.axis_index("narrow")
    rounds, narrow, wide, _, strip, lanes = grid_ref.shape
    windows = (window_a, window_b)
    slots = x_ref.shape[0]
    block_y, width = scale_ref.shape
    slabs, samples, cells = cross_ref.shape
    pitch = depth + 1
    half = wide * strip
    span = cells // depth

    core = lax.rem(w, 2)
    across = w + 2 - 4 * lax.rem(lax.div(w, 2), 2)
    along = w + 4 - 8 * lax.rem(lax.div(w, 4), 2)
    first = across + core * (along - across)
    second = along + core * (across - along)
    corner = across + along - w
    sibling = w + 1 - 2 * core
    held = (w, first, second, corner)
    straight = ((0, 3),)
    sib_across = across + 1 - 2 * core
    sib_along = along + 1 - 2 * core
    sib_first = sib_along + core * (sib_across - sib_along)
    sib_second = sib_across + core * (sib_along - sib_across)
    theirs = (sibling, sib_first, sib_second, corner + 1 - 2 * core)

    def remote(source, place, send, receive, target):
        return pltpu.make_async_remote_copy(
            src_ref=source, dst_ref=place, send_sem=send, recv_sem=receive,
            device_id=target, device_id_type=pl.DeviceIdType.MESH,
        )

    image_loads = [
        pltpu.make_async_copy(
            image_hbm.at[:, r * strip : (r + 1) * strip],
            image_ref.at[:, r * strip : (r + 1) * strip],
            image_sem.at[r],
        )
        for r in range(rounds)
    ]
    table_loads = [
        pltpu.make_async_copy(source, place, table_sem.at[i])
        for i, (source, place) in enumerate(((z_hbm, z_ref), (row_hbm, packed_ref), (line_hbm, line_ref)))
    ]

    def x_load(s):
        return pltpu.make_async_copy(x_hbm.at[s], x_ref.at[s % slots], x_sem.at[s % slots])

    def cross_load(s):
        return pltpu.make_async_copy(cross_hbm.at[s], cross_ref.at[s], cross_sem.at[s])

    small_loads = [
        pltpu.make_async_copy(source, place, small_sem.at[i])
        for i, (source, place) in enumerate(((deap_hbm, deap_smem), (deap_hbm, deap_ref), (offsets_hbm, offsets_ref)))
    ]
    for copy in small_loads:
        copy.start()
    image_loads[0].start()
    table_loads[0].start()
    image_loads[1].start()
    barrier = pltpu.get_barrier_semaphore()
    peers = [(w, flip(n, j)) for j in range(1, narrow)] + [(first, n), (second, n), (corner, n), (sibling, n)]
    for peer in peers:
        pl.semaphore_signal(barrier, inc=1, device_id=peer, device_id_type=pl.DeviceIdType.MESH)

    row_at = lax.broadcasted_iota(jnp.int32, perm_ref.shape, 0)
    lane_at = lax.broadcasted_iota(jnp.int32, perm_ref.shape, 1)
    parity_at = lax.rem(lax.div(lax.rem(lane_at, lanes), block_y) + n, 2)
    line_at = lax.div(lax.rem(lane_at, block_y), block_y // 2)
    source_at = lax.div(lane_at, lanes) * lanes + line_at * block_y + 2 * lax.rem(lane_at, block_y // 2) + parity_at
    perm_ref[...] = jnp.where(row_at == source_at, 1.0, 0.0).astype(jnp.bfloat16)
    for copy in small_loads:
        copy.wait()
    last = deap_ref[2:3, :]
    for y in range(block_y):
        scale_ref[y : y + 1, :] = last * deap_smem[1, n * block_y + y]

    def band(r):
        quarter = block_y // 2
        low = lax.rem(lax.broadcasted_iota(jnp.int32, (narrow * depth, lanes), 1), block_y) < quarter
        group = width // block_y
        rows = 2 * narrow * depth
        halves = []
        for c in range(2):
            pieces = []
            for x in range(strip):
                gain = scale_ref[...] * deap_smem[0, w * rounds * strip + r * strip + x]
                pieces.append((image_ref[c, r * strip + x].astype(jnp.float32) * gain).astype(jnp.bfloat16))
            halves.append(jnp.concatenate(pieces, axis=0))
        both = jnp.concatenate(halves, axis=1)
        value = lax.dot_general(z_ref[...], both, (((1,), (1,)), ((), ())), preferred_element_type=jnp.float32)
        value = value.astype(jnp.bfloat16)
        value = jnp.concatenate([value[:, at : at + width] for at in range(0, strip * block_y, width)], axis=0)
        value = jnp.dot(value, perm_ref[...], preferred_element_type=jnp.float32)
        for at in range(0, strip, group):
            real = value[at // group * rows : at // group * rows + rows // 2]
            imag = value[at // group * rows + rows // 2 : (at // group + 1) * rows]
            for pair in range(group // 2):
                here = slice(pair * lanes, (pair + 1) * lanes)
                even = jnp.where(low, real[:, here], pltpu.roll(imag[:, here], quarter, 1))
                odd = jnp.where(low, pltpu.roll(real[:, here], lanes - quarter, 1), imag[:, here])
                spread_ref[pl.ds(at + 2 * pair, narrow * depth, stride=pitch), :] = even
                spread_ref[pl.ds(at + 2 * pair + 1, narrow * depth, stride=pitch), :] = odd
        for k in range(narrow * depth):
            send_ref[r, k // depth, k % depth] = spread_ref[k * pitch : k * pitch + strip, :].astype(jnp.bfloat16)
        grid_ref[r, n, w] = send_ref[r, n]

    def swap(r, j):
        peer = flip(n, j)
        return remote(
            send_ref.at[r, peer], grid_ref.at[r, n, w], swap_send.at[r, j], swap_recv.at[r, j], (w, peer)
        )

    def place(r, j, column):
        return grid_ref.at[r, flip(n, j), column]

    def own_copies(r, j):
        mine = place(r, j, w)
        return [
            remote(mine, mine, own_send.at[r, j, 0], near_recv.at[r, j, 0], (first, n)),
            remote(mine, mine, own_send.at[r, j, 1], near_recv.at[r, j, 1], (second, n)),
            pass_copy(r, j, 0),
        ]

    def relay_copy(r, j):
        column, target = (w, corner) if (r, j) in straight else (first, second)
        block = place(r, j, column)
        return remote(block, block, relay_send.at[r, j], relay_recv.at[r, j], (target, n))

    def pass_copy(r, j, kind):
        block = place(r, j, held[kind])
        return remote(block, block, pass_send.at[r, j, kind], pass_recv.at[r, j, kind], (sibling, n))

    def arrived(r, j, column, send, receive):
        block = place(r, j, column)
        remote(block, block, send, receive, (sibling, n)).wait_recv()

    def own(r, j):
        if j > 0:
            block = grid_ref.at[r, flip(n, j), w]
            remote(block, block, swap_send.at[r, j], swap_recv.at[r, j], (w, flip(n, j))).wait_recv()
        for copy in own_copies(r, j):
            copy.start()
        if (r, j) in straight:
            relay_copy(r, j).start()

    def relay(r, j):
        arrived(r, j, first, own_send.at[r, j, 0], near_recv.at[r, j, 0])
        if (r, j) not in straight:
            relay_copy(r, j).start()
        pass_copy(r, j, 1).start()

    def near(r, j):
        arrived(r, j, second, own_send.at[r, j, 1], near_recv.at[r, j, 1])
        pass_copy(r, j, 2).start()

    def far(r, j):
        arrived(r, j, corner, relay_send.at[r, j], relay_recv.at[r, j])
        pass_copy(r, j, 3).start()

    def settle(r):
        for j in range(narrow):
            for kind in range(4):
                arrived(r, j, theirs[kind], pass_send.at[r, j, kind], pass_recv.at[r, j, kind])

    def gains(*batch):
        for s in batch:
            x_load(s).wait()
        for s, window in zip(batch, windows):
            start = offsets_ref[0, s]
            for block in range(row_ref.shape[0]):
                window[:, block * 128 : (block + 1) * 128] = row_ref[block, pl.ds(start, BX), :].astype(jnp.bfloat16)
            for at in range(0, samples, 512):
                rows = slice(at, at + 512)
                gain_ref[s, rows] = jnp.dot(
                    x_ref[s % slots, rows], window[...], preferred_element_type=jnp.float32
                ).astype(jnp.bfloat16)
        for s in batch:
            if s + slots < slabs:
                x_load(s + slots).start()
        for s in batch:
            cross_load(s).start()

    def lines(r, k):
        low = lax.broadcasted_iota(jnp.int32, (2 * half, lanes), 1) < block_y
        planes = [
            jnp.concatenate([grid_ref[r, source, :, k + i].reshape(half, lanes) for i in range(2)], axis=0)
            for source in range(narrow)
        ]
        evens, odds = [], []
        for one, two in zip(planes[::2], planes[1::2]):
            evens.append(jnp.where(low, one, two))
            odds.append(jnp.where(low, two, one))
        even, odd = [
            lax.dot_general(
                line_ref[parity], jnp.concatenate(pieces, axis=1), (((1,), (1,)), ((), ())),
                preferred_element_type=jnp.float32,
            )
            for parity, pieces in enumerate((evens, odds))
        ]
        for sign, value in enumerate((even + odd, even - odd)):
            for part in range(2):
                for i in range(2):
                    wide_ref[part, pl.ds(sign * (grid_rows // 2) * pitch + k + i, grid_rows // 2, stride=pitch), :] = value[
                        part * grid_rows // 2 : (part + 1) * grid_rows // 2, i * half : (i + 1) * half
                    ]

    def gather(s, slab_ref):
        base = s * span * pitch
        for part in range(2):
            for y in range(span):
                slab_ref[y * depth : (y + 1) * depth, part * half : (part + 1) * half] = wide_ref[
                    part, pl.ds(base + y * pitch, depth), :
                ].astype(jnp.bfloat16)

    def contract(r, s, slab_ref):
        for at in range(0, samples, tile):
            rows = slice(at, at + tile)
            value = jnp.dot(cross_ref[s, rows], slab_ref[...], preferred_element_type=jnp.float32)
            real, imag = value[:, :half], value[:, half:]
            gain = gain_ref[s, rows, 2 * r * half : 2 * (r + 1) * half].astype(jnp.float32)
            cosine, sine = gain[:, :half], gain[:, half:]
            for part, product in enumerate((cosine * real + sine * imag, cosine * imag - sine * real)):
                total = jnp.sum(product.T, axis=0, keepdims=True)
                if r > 0:
                    total = total + out_ref[s, part : part + 1, rows]
                out_ref[s, part : part + 1, rows] = total

    for copy in table_loads[1:]:
        copy.start()
    for s in range(slots):
        x_load(s).start()
    table_loads[0].wait()
    image_loads[0].wait()
    band(0)
    pl.semaphore_wait(barrier, len(peers))
    for j in range(1, narrow):
        swap(0, j).start()
    own(0, 0)
    image_loads[1].wait()
    band(1)
    own(1, 0)
    table_loads[1].wait()
    row_ref[...] = packed_ref[...].astype(jnp.float32)
    gains(0, 1)
    relay(0, 0)
    own(0, 1)
    gains(2, 3)
    near(0, 0)
    own(0, 2)
    gains(4, 5)
    own(0, 3)
    for j in range(1, narrow):
        swap(1, j).start()
    relay(0, 1)
    near(0, 1)
    far(0, 0)
    gains(6, 7)
    relay(0, 2)
    near(0, 2)
    relay(0, 3)
    near(0, 3)
    far(0, 1)
    relay(1, 0)
    near(1, 0)
    far(0, 2)
    far(0, 3)
    own(1, 1)
    settle(0)
    own(1, 2)
    table_loads[2].wait()
    for pair in range(depth // 2):
        lines(0, 2 * pair)
    own(1, 3)
    for s in range(slabs):
        cross_load(s).wait()

    events = (
        ((far, 0), (relay, 1), (near, 1)),
        ((relay, 2), (near, 2), (far, 1), (relay, 3), (near, 3)),
        ((far, 2), (far, 3)),
    )

    def steps(r, i):
        gather(2 * i + 1, slab_b)
        contract(r, 2 * i, slab_a)
        gather(lax.rem(2 * i + 2, slabs), slab_a)
        contract(r, 2 * i + 1, slab_b)

    def early(i, carry):
        steps(0, i)
        for at, batch in enumerate(events):

            @pl.when(i == at)
            def _():
                for event, j in batch:
                    event(1, j)

        return carry

    def late(i, carry):
        steps(1, 2 * i)
        steps(1, 2 * i + 1)
        return carry

    gather(0, slab_a)
    lax.fori_loop(0, slabs // 2, early, 0)
    settle(1)
    for pair in range(depth // 2):
        lines(1, 2 * pair)
    gather(0, slab_a)
    lax.fori_loop(0, slabs // 4, late, 0)

    for r in range(rounds):
        for j in range(narrow):
            if j > 0:
                swap(r, j).wait_send()
            for copy in own_copies(r, j):
                copy.wait_send()
            relay_copy(r, j).wait_send()
            for kind in range(1, 4):
                pass_copy(r, j, kind).wait_send()


def fused_device(image, deapodization, offsets, cross_weight, x_weight):
    wide = lax.axis_size("wide")
    narrow = lax.axis_size("narrow")
    block_x, block_y, width = image.shape[1:]
    depth = KZ // narrow
    slabs, samples, cells = cross_weight.shape[1:]
    rounds = 2
    strip = block_x // rounds
    lanes = 2 * block_y
    slots = 4
    z_table = complex_table(*base_tables(KZ, width, G, -(KZ // 2))).reshape(2 * KZ, 2 * width)
    cosine, sine = base_tables(G, width, G, -(G // 2))
    line_table = complex_table(cosine[: G // 2], sine[: G // 2]).reshape(G, 2, narrow, block_y // 2, 2)
    line_table = line_table.transpose(4, 0, 2, 1, 3)
    swapped = line_table[1].reshape(G, narrow // 2, 2, lanes // 2)[:, :, ::-1]
    line_table = np.stack([line_table[0].reshape(G, width), swapped.reshape(G, width)])
    row_table = np.stack([cosine, sine], axis=0).reshape(2, G, wide, rounds, strip)
    row_table = row_table.transpose(3, 0, 1, 2, 4).reshape(2 * rounds, G, wide * strip)
    hbm = pl.BlockSpec(memory_space=pl.ANY)
    vmem = pl.BlockSpec(memory_space=pltpu.VMEM)
    dma = pltpu.SemaphoreType.DMA
    half = wide * strip
    out = pl.pallas_call(
        functools.partial(fused_kernel, (depth, G, TILE if samples % TILE == 0 else samples)),
        out_shape=jax.ShapeDtypeStruct((slabs, 2, samples), jnp.float32),
        in_specs=[hbm] * 8,
        out_specs=vmem,
        scratch_shapes=[
            pltpu.SMEM(deapodization.shape, jnp.float32),
            pltpu.VMEM(deapodization.shape, jnp.float32),
            pltpu.SMEM(offsets.shape, jnp.int32),
            pltpu.VMEM(image.shape, jnp.bfloat16),
            pltpu.VMEM((block_y, width), jnp.float32),
            pltpu.VMEM((width, width), jnp.bfloat16),
            pltpu.VMEM((KZ * (depth + 1), lanes), jnp.float32),
            pltpu.VMEM((rounds, narrow, depth, strip, lanes), jnp.bfloat16),
            pltpu.VMEM((rounds, narrow, wide, depth, strip, lanes), jnp.bfloat16),
            pltpu.VMEM(z_table.shape, jnp.bfloat16),
            pltpu.VMEM(line_table.shape, jnp.bfloat16),
            pltpu.VMEM(row_table.shape, jnp.bfloat16),
            pltpu.VMEM(row_table.shape, jnp.float32),
            pltpu.VMEM((slots, samples, BX), jnp.bfloat16),
            pltpu.VMEM((BX, 2 * width), jnp.bfloat16),
            pltpu.VMEM((BX, 2 * width), jnp.bfloat16),
            pltpu.VMEM((slabs, samples, 2 * width), jnp.bfloat16),
            pltpu.VMEM((slabs, samples, cells), jnp.bfloat16),
            pltpu.VMEM((2, G * (depth + 1), half), jnp.float32),
            pltpu.VMEM((cells, 2 * half), jnp.bfloat16),
            pltpu.VMEM((cells, 2 * half), jnp.bfloat16),
            dma((3,)),
            dma((rounds,)),
            dma((3,)),
            dma((slots,)),
            dma((slabs,)),
            dma((rounds, narrow)),
            dma((rounds, narrow)),
            dma((rounds, narrow, 2)),
            dma((rounds, narrow, 2)),
            dma((rounds, narrow)),
            dma((rounds, narrow)),
            dma((rounds, narrow, 4)),
            dma((rounds, narrow, 4)),
        ],
        compiler_params=pltpu.CompilerParams(
            vmem_limit_bytes=67043328 - 100 * 1024, collective_id=1, has_side_effects=True
        ),
    )(
        image, deapodization, offsets, jnp.asarray(z_table), jnp.asarray(line_table),
        jnp.asarray(row_table), x_weight[0], cross_weight[0],
    )
    return out[None]


def solution(mesh):
    square = mesh.shape["wide"] == 8 and mesh.shape["narrow"] == 4
    return jax.shard_map(
        fused_device if square else per_device,
        mesh=mesh,
        in_specs=(
            P(None, "wide", "narrow", None),
            P(),
            P(("wide", "narrow"), None),
            P(("wide", "narrow"), None, None, None),
            P(("wide", "narrow"), None, None, None),
        ),
        out_specs=P(("wide", "narrow"), None, None, None),
        check_vma=False,
    )
```

```python
import functools
import math

import jax
import jax.numpy as jnp
import numpy as np
from jax import lax
from jax.experimental import pallas as pl
from jax.experimental.pallas import tpu as pltpu
from jax.sharding import PartitionSpec as P

G = 512
KZ = 64
BX = 256
TILE = 128


def base_tables(out_rows, inputs, grid_size, lowest):
    frequency = np.arange(out_rows, dtype=np.int64) + lowest
    position = np.arange(inputs, dtype=np.int64) - inputs // 2
    phases = np.mod(frequency[:, None] * position[None, :], grid_size)
    angles = phases.astype(np.float64) * (2.0 * math.pi / grid_size)
    factor = 1.0 / math.sqrt(inputs)
    cosine = (np.cos(angles) * factor).astype(np.float32).astype(jnp.bfloat16)
    sine = (np.sin(angles) * factor).astype(np.float32).astype(jnp.bfloat16)
    return cosine, sine


def complex_table(cosine, sine):
    real_rows = np.stack([cosine, sine], axis=1)
    imag_rows = np.stack([-sine, cosine], axis=1)
    return np.stack([real_rows, imag_rows], axis=0)


def sample_kernel(
    sizes, offsets_ref, band_ref, line_ref, row_ref, x_ref, cross_ref, out_ref, wide_ref, slab_ref, window_ref
):
    depth, grid_rows, width, tile = sizes
    step = pl.program_id(0)
    cells = slab_ref.shape[0]

    @pl.when(step == 0)
    def _():
        def one_plane(k, carry):
            parts = [
                band_ref[:, piece, k].reshape(width, band_ref.shape[-1])
                for piece in range(band_ref.shape[1])
            ]
            plane = jnp.concatenate(parts, axis=-1) if len(parts) > 1 else parts[0]
            lines = lax.dot_general(
                line_ref[...], plane, (((1,), (1,)), ((), ())), preferred_element_type=jnp.float32
            )
            for part in range(2):
                for lane in range(0, width, 128):
                    wide_ref[(part * width + lane) // 128, pl.ds(k, grid_rows, stride=depth), :] = lines[
                        part * grid_rows : (part + 1) * grid_rows, lane : lane + 128
                    ]
            return carry

        for k in range(depth):
            one_plane(k, 0)

    here = pl.ds(pl.multiple_of(step * cells, cells), cells)
    start = offsets_ref[0, step]
    for block in range(2 * width // 128):
        lanes = slice(block * 128, (block + 1) * 128)
        slab_ref[:, lanes] = wide_ref[block, here, :].astype(jnp.bfloat16)
        window_ref[:, lanes] = row_ref[block, pl.ds(start, BX), :].astype(jnp.bfloat16)
    for first in range(0, cross_ref.shape[1], tile):
        rows = slice(first, first + tile)
        partial = jnp.dot(cross_ref[0, rows], slab_ref[...], preferred_element_type=jnp.float32)
        gain = jnp.dot(x_ref[0, rows], window_ref[...], preferred_element_type=jnp.float32)
        part_re, part_im = partial[:, :width], partial[:, width:]
        gain_cos, gain_sin = gain[:, :width], gain[:, width:]
        for part, value in enumerate(
            (gain_cos * part_re + gain_sin * part_im, gain_cos * part_im - gain_sin * part_re)
        ):
            folded = value[:, :128]
            for lane in range(128, width, 128):
                folded = folded + value[:, lane : lane + 128]
            out_ref[0, part : part + 1, rows] = jnp.sum(folded.T, axis=0, keepdims=True)


def gather_kernel(
    wide, narrow, band_ref, out_ref, own_sem, swap_send, swap_recv, chip_send, chip_recv, core_send, core_recv
):
    w = lax.axis_index("wide")
    n = lax.axis_index("narrow")
    sibling = w + 1 - 2 * lax.rem(w, 2)
    chips = wide // 2
    barrier = pltpu.get_barrier_semaphore()
    targets = [(w, lax.rem(n + j, narrow)) for j in range(1, narrow)]
    targets += [(lax.rem(w + 2 * j, wide), n) for j in range(1, chips)] + [(sibling, n)]
    for target in targets:
        pl.semaphore_signal(
            barrier, inc=1, device_id=target, device_id_type=pl.DeviceIdType.MESH
        )
    pl.semaphore_wait(barrier, len(targets))

    def remote(source, place, send, receive, target):
        return pltpu.make_async_remote_copy(
            src_ref=source,
            dst_ref=place,
            send_sem=send,
            recv_sem=receive,
            device_id=target,
            device_id_type=pl.DeviceIdType.MESH,
        )

    swaps = []
    for j in range(1, narrow):
        peer = lax.rem(n + j, narrow)
        swap = remote(
            band_ref.at[peer], out_ref.at[w, n], swap_send.at[j - 1], swap_recv.at[j - 1], (w, peer)
        )
        swap.start()
        swaps.append(swap)
    own = pltpu.make_async_copy(band_ref.at[n], out_ref.at[w, n], own_sem)
    own.start()
    own.wait()
    for swap in swaps:
        swap.wait()
    mine = out_ref.at[w]
    hops = []
    for j in range(1, chips):
        peer = lax.rem(w + 2 * j, wide)
        hop = remote(mine, mine, chip_send.at[j - 1], chip_recv.at[j - 1], (peer, n))
        hop.start()
        hops.append(hop)
    passes = [remote(mine, mine, core_send.at[0], core_recv.at[0], (sibling, n))]
    passes[0].start()
    for j in range(1, chips):
        hops[j - 1].wait_recv()
        block = out_ref.at[lax.rem(w + wide - 2 * j, wide)]
        forward = remote(block, block, core_send.at[j], core_recv.at[j], (sibling, n))
        forward.start()
        passes.append(forward)
    for hop in hops:
        hop.wait_send()
    for forward in passes:
        forward.wait()


def per_device(image, deapodization, offsets, cross_weight, x_weight):
    wide_count = lax.axis_size("wide")
    narrow_count = lax.axis_size("narrow")
    wide_index = lax.axis_index("wide")
    narrow_index = lax.axis_index("narrow")
    block_x = image.shape[1]
    block_y = image.shape[2]
    width = image.shape[3]
    depth = KZ // narrow_count
    samples, cells = cross_weight.shape[2], cross_weight.shape[3]
    scale_x = lax.dynamic_slice_in_dim(deapodization[0], wide_index * block_x, block_x)
    scale_y = lax.dynamic_slice_in_dim(deapodization[1], narrow_index * block_y, block_y)
    weighted = (
        image.astype(jnp.float32)
        * scale_x[None, :, None, None]
        * scale_y[None, None, :, None]
        * deapodization[2][None, None, None, :]
    ).astype(jnp.bfloat16)
    z_table = complex_table(*base_tables(KZ, width, G, -(KZ // 2)))
    band = jnp.einsum(
        "okcz,cxyz->kxoy", jnp.asarray(z_table), weighted, preferred_element_type=jnp.float32
    ).astype(jnp.bfloat16)
    band = band.reshape(KZ, block_x, 2 * block_y)
    band = band.reshape(narrow_count, depth, block_x, 2 * block_y)
    chips = wide_count // 2
    band = pl.pallas_call(
        functools.partial(gather_kernel, wide_count, narrow_count),
        out_shape=jax.ShapeDtypeStruct((wide_count,) + band.shape, band.dtype),
        in_specs=[pl.BlockSpec(memory_space=pltpu.VMEM)],
        out_specs=pl.BlockSpec(memory_space=pltpu.VMEM),
        scratch_shapes=[
            pltpu.SemaphoreType.DMA,
            pltpu.SemaphoreType.DMA((narrow_count - 1,)),
            pltpu.SemaphoreType.DMA((narrow_count - 1,)),
            pltpu.SemaphoreType.DMA((chips - 1,)),
            pltpu.SemaphoreType.DMA((chips - 1,)),
            pltpu.SemaphoreType.DMA((chips,)),
            pltpu.SemaphoreType.DMA((chips,)),
        ],
        compiler_params=pltpu.CompilerParams(collective_id=0, has_side_effects=True),
    )(band)
    if (2 * block_y) % 128:
        band = band.transpose(0, 2, 3, 1, 4).reshape(wide_count, 1, depth, block_x, 2 * width)

    cosine, sine = base_tables(G, width, G, -(G // 2))
    line_table = complex_table(cosine, sine).reshape(2 * G, 2, narrow_count, block_y)
    line_table = line_table.transpose(0, 2, 1, 3).reshape(2 * G, 2 * width)
    row_table = np.concatenate([cosine, sine], axis=1).astype(np.float32)
    row_table = row_table.reshape(G, 2 * width // 128, 128).transpose(1, 0, 2)

    tile = 512 if samples % 512 == 0 else samples
    kernel = functools.partial(sample_kernel, (depth, G, width, tile))
    out = pl.pallas_call(
        kernel,
        grid=(wide_count,),
        out_shape=jax.ShapeDtypeStruct((wide_count, 2, samples), jnp.float32),
        in_specs=[
            pl.BlockSpec(memory_space=pltpu.SMEM),
            pl.BlockSpec(band.shape, lambda s: (0, 0, 0, 0, 0)),
            pl.BlockSpec(line_table.shape, lambda s: (0, 0)),
            pl.BlockSpec(row_table.shape, lambda s: (0, 0, 0)),
            pl.BlockSpec((1, samples, BX), lambda s: (s, 0, 0)),
            pl.BlockSpec((1, samples, cells), lambda s: (s, 0, 0)),
        ],
        out_specs=pl.BlockSpec((1, 2, samples), lambda s: (s, 0, 0)),
        scratch_shapes=[
            pltpu.VMEM((2 * width // 128, G * depth, 128), jnp.float32),
            pltpu.VMEM((cells, 2 * width), jnp.bfloat16),
            pltpu.VMEM((BX, 2 * width), jnp.bfloat16),
        ],
        compiler_params=pltpu.CompilerParams(vmem_limit_bytes=60 * 1024 * 1024),
        cost_estimate=pl.CostEstimate(
            flops=2 * wide_count * samples * 2 * width * (cells + BX) + 8 * G * width * width * depth,
            bytes_accessed=2 * wide_count * samples * (cells + BX),
            transcendentals=0,
        ),
    )(offsets, band, jnp.asarray(line_table), jnp.asarray(row_table), x_weight[0], cross_weight[0])
    return out[None]


def flip(index, bits):
    low = lax.rem(index + bits, 2)
    high = lax.rem(lax.div(index, 2) + lax.div(bits, 2), 2)
    return low + 2 * high


def fused_kernel(
    sizes, image_hbm, deap_hbm, offsets_hbm, z_hbm, line_hbm, row_hbm, x_hbm, cross_hbm, out_ref,
    deap_smem, deap_ref, offsets_ref, image_ref, scale_ref, perm_ref, spread_ref, send_ref, grid_ref, z_ref, line_ref, packed_ref, row_ref, x_ref, window_a, window_b, gain_ref,
    cross_ref, wide_ref, slab_a, slab_b,
    small_sem, image_sem, table_sem, x_sem, cross_sem,
    swap_send, swap_recv, own_send, near_recv, relay_send, relay_recv, pass_send, pass_recv,
):
    depth, grid_rows, tile = sizes
    w = lax.axis_index("wide")
    n = lax.axis_index("narrow")
    rounds, narrow, wide, _, strip, lanes = grid_ref.shape
    windows = (window_a, window_b)
    slots = x_ref.shape[0]
    block_y, width = scale_ref.shape
    slabs, samples, cells = cross_ref.shape
    pitch = depth + 1
    half = wide * strip
    span = cells // depth

    core = lax.rem(w, 2)
    across = w + 2 - 4 * lax.rem(lax.div(w, 2), 2)
    along = w + 4 - 8 * lax.rem(lax.div(w, 4), 2)
    first = across + core * (along - across)
    second = along + core * (across - along)
    corner = across + along - w
    sibling = w + 1 - 2 * core
    held = (w, first, second, corner)
    straight = ((0, 3), (1, 3))
    sib_across = across + 1 - 2 * core
    sib_along = along + 1 - 2 * core
    sib_first = sib_along + core * (sib_across - sib_along)
    sib_second = sib_across + core * (sib_along - sib_across)
    theirs = (sibling, sib_first, sib_second, corner + 1 - 2 * core)

    def remote(source, place, send, receive, target):
        return pltpu.make_async_remote_copy(
            src_ref=source, dst_ref=place, send_sem=send, recv_sem=receive,
            device_id=target, device_id_type=pl.DeviceIdType.MESH,
        )

    image_loads = [
        pltpu.make_async_copy(
            image_hbm.at[:, r * strip : (r + 1) * strip],
            image_ref.at[:, r * strip : (r + 1) * strip],
            image_sem.at[r],
        )
        for r in range(rounds)
    ]
    table_loads = [
        pltpu.make_async_copy(source, place, table_sem.at[i])
        for i, (source, place) in enumerate(((z_hbm, z_ref), (row_hbm, packed_ref), (line_hbm, line_ref)))
    ]

    def x_load(s):
        return pltpu.make_async_copy(x_hbm.at[s], x_ref.at[s % slots], x_sem.at[s % slots])

    def cross_load(s):
        return pltpu.make_async_copy(cross_hbm.at[s], cross_ref.at[s], cross_sem.at[s])

    small_loads = [
        pltpu.make_async_copy(source, place, small_sem.at[i])
        for i, (source, place) in enumerate(((deap_hbm, deap_smem), (deap_hbm, deap_ref), (offsets_hbm, offsets_ref)))
    ]
    for copy in small_loads:
        copy.start()
    image_loads[0].start()
    table_loads[0].start()
    image_loads[1].start()
    barrier = pltpu.get_barrier_semaphore()
    peers = [(w, flip(n, j)) for j in range(1, narrow)] + [(first, n), (second, n), (corner, n), (sibling, n)]
    for peer in peers:
        pl.semaphore_signal(barrier, inc=1, device_id=peer, device_id_type=pl.DeviceIdType.MESH)

    row_at = lax.broadcasted_iota(jnp.int32, perm_ref.shape, 0)
    lane_at = lax.broadcasted_iota(jnp.int32, perm_ref.shape, 1)
    parity_at = lax.rem(lax.div(lax.rem(lane_at, lanes), block_y) + n, 2)
    line_at = lax.div(lax.rem(lane_at, block_y), block_y // 2)
    source_at = lax.div(lane_at, lanes) * lanes + line_at * block_y + 2 * lax.rem(lane_at, block_y // 2) + parity_at
    perm_ref[...] = jnp.where(row_at == source_at, 1.0, 0.0).astype(jnp.bfloat16)
    for copy in small_loads:
        copy.wait()
    last = deap_ref[2:3, :]
    for y in range(block_y):
        scale_ref[y : y + 1, :] = last * deap_smem[1, n * block_y + y]

    def band(r):
        quarter = block_y // 2
        low = lax.rem(lax.broadcasted_iota(jnp.int32, (narrow * depth, lanes), 1), block_y) < quarter
        group = width // block_y
        rows = 2 * narrow * depth
        halves = []
        for c in range(2):
            pieces = []
            for x in range(strip):
                gain = scale_ref[...] * deap_smem[0, w * rounds * strip + r * strip + x]
                pieces.append((image_ref[c, r * strip + x].astype(jnp.float32) * gain).astype(jnp.bfloat16))
            halves.append(jnp.concatenate(pieces, axis=0))
        both = jnp.concatenate(halves, axis=1)
        value = lax.dot_general(z_ref[...], both, (((1,), (1,)), ((), ())), preferred_element_type=jnp.float32)
        value = value.astype(jnp.bfloat16)
        value = jnp.concatenate([value[:, at : at + width] for at in range(0, strip * block_y, width)], axis=0)
        value = jnp.dot(value, perm_ref[...], preferred_element_type=jnp.float32)
        for at in range(0, strip, group):
            real = value[at // group * rows : at // group * rows + rows // 2]
            imag = value[at // group * rows + rows // 2 : (at // group + 1) * rows]
            for pair in range(group // 2):
                here = slice(pair * lanes, (pair + 1) * lanes)
                even = jnp.where(low, real[:, here], pltpu.roll(imag[:, here], quarter, 1))
                odd = jnp.where(low, pltpu.roll(real[:, here], lanes - quarter, 1), imag[:, here])
                spread_ref[pl.ds(at + 2 * pair, narrow * depth, stride=pitch), :] = even
                spread_ref[pl.ds(at + 2 * pair + 1, narrow * depth, stride=pitch), :] = odd
        for k in range(narrow * depth):
            send_ref[r, k // depth, k % depth] = spread_ref[k * pitch : k * pitch + strip, :].astype(jnp.bfloat16)
        grid_ref[r, n, w] = send_ref[r, n]

    def swap(r, j):
        peer = flip(n, j)
        return remote(
            send_ref.at[r, peer], grid_ref.at[r, n, w], swap_send.at[r, j], swap_recv.at[r, j], (w, peer)
        )

    def place(r, j, column):
        return grid_ref.at[r, flip(n, j), column]

    def own_copies(r, j):
        mine = place(r, j, w)
        return [
            remote(mine, mine, own_send.at[r, j, 0], near_recv.at[r, j, 0], (first, n)),
            remote(mine, mine, own_send.at[r, j, 1], near_recv.at[r, j, 1], (second, n)),
            pass_copy(r, j, 0),
        ]

    def relay_copy(r, j):
        column, target = (w, corner) if (r, j) in straight else (first, second)
        block = place(r, j, column)
        return remote(block, block, relay_send.at[r, j], relay_recv.at[r, j], (target, n))

    def pass_copy(r, j, kind):
        block = place(r, j, held[kind])
        return remote(block, block, pass_send.at[r, j, kind], pass_recv.at[r, j, kind], (sibling, n))

    def arrived(r, j, column, send, receive):
        block = place(r, j, column)
        remote(block, block, send, receive, (sibling, n)).wait_recv()

    def own(r, j):
        if j > 0:
            block = grid_ref.at[r, flip(n, j), w]
            remote(block, block, swap_send.at[r, j], swap_recv.at[r, j], (w, flip(n, j))).wait_recv()
        for copy in own_copies(r, j):
            copy.start()
        if (r, j) in straight:
            relay_copy(r, j).start()

    def relay(r, j):
        arrived(r, j, first, own_send.at[r, j, 0], near_recv.at[r, j, 0])
        if (r, j) not in straight:
            relay_copy(r, j).start()
        pass_copy(r, j, 1).start()

    def near(r, j):
        arrived(r, j, second, own_send.at[r, j, 1], near_recv.at[r, j, 1])
        pass_copy(r, j, 2).start()

    def far(r, j):
        arrived(r, j, corner, relay_send.at[r, j], relay_recv.at[r, j])
        pass_copy(r, j, 3).start()

    def settle(r):
        for j in range(narrow):
            for kind in range(4):
                arrived(r, j, theirs[kind], pass_send.at[r, j, kind], pass_recv.at[r, j, kind])

    def gains(*batch):
        for s in batch:
            x_load(s).wait()
        for s, window in zip(batch, windows):
            start = offsets_ref[0, s]
            for block in range(row_ref.shape[0]):
                window[:, block * 128 : (block + 1) * 128] = row_ref[block, pl.ds(start, BX), :].astype(jnp.bfloat16)
            for at in range(0, samples, 512):
                rows = slice(at, at + 512)
                gain_ref[s, rows] = jnp.dot(
                    x_ref[s % slots, rows], window[...], preferred_element_type=jnp.float32
                ).astype(jnp.bfloat16)
        for s in batch:
            if s + slots < slabs:
                x_load(s + slots).start()
        for s in batch:
            cross_load(s).start()

    def lines(r, k):
        low = lax.broadcasted_iota(jnp.int32, (2 * half, lanes), 1) < block_y
        planes = [
            jnp.concatenate([grid_ref[r, source, :, k + i].reshape(half, lanes) for i in range(2)], axis=0)
            for source in range(narrow)
        ]
        evens, odds = [], []
        for one, two in zip(planes[::2], planes[1::2]):
            evens.append(jnp.where(low, one, two))
            odds.append(jnp.where(low, two, one))
        even, odd = [
            lax.dot_general(
                line_ref[parity], jnp.concatenate(pieces, axis=1), (((1,), (1,)), ((), ())),
                preferred_element_type=jnp.float32,
            )
            for parity, pieces in enumerate((evens, odds))
        ]
        for sign, value in enumerate((even + odd, even - odd)):
            for part in range(2):
                for i in range(2):
                    wide_ref[part, pl.ds(sign * (grid_rows // 2) * pitch + k + i, grid_rows // 2, stride=pitch), :] = value[
                        part * grid_rows // 2 : (part + 1) * grid_rows // 2, i * half : (i + 1) * half
                    ]

    def gather(s, slab_ref):
        base = s * span * pitch
        for part in range(2):
            for y in range(span):
                slab_ref[y * depth : (y + 1) * depth, part * half : (part + 1) * half] = wide_ref[
                    part, pl.ds(base + y * pitch, depth), :
                ].astype(jnp.bfloat16)

    def contract(r, s, slab_ref):
        for at in range(0, samples, tile):
            rows = slice(at, at + tile)
            value = jnp.dot(cross_ref[s, rows], slab_ref[...], preferred_element_type=jnp.float32)
            real, imag = value[:, :half], value[:, half:]
            gain = gain_ref[s, rows, 2 * r * half : 2 * (r + 1) * half].astype(jnp.float32)
            cosine, sine = gain[:, :half], gain[:, half:]
            for part, product in enumerate((cosine * real + sine * imag, cosine * imag - sine * real)):
                total = jnp.sum(product.T, axis=0, keepdims=True)
                if r > 0:
                    total = total + out_ref[s, part : part + 1, rows]
                out_ref[s, part : part + 1, rows] = total

    for copy in table_loads[1:]:
        copy.start()
    for s in range(slots):
        x_load(s).start()
    table_loads[0].wait()
    image_loads[0].wait()
    band(0)
    pl.semaphore_wait(barrier, len(peers))
    for j in range(1, narrow):
        swap(0, j).start()
    own(0, 0)
    image_loads[1].wait()
    band(1)
    own(1, 0)
    table_loads[1].wait()
    row_ref[...] = packed_ref[...].astype(jnp.float32)
    gains(0, 1)
    relay(0, 0)
    own(0, 1)
    gains(2, 3)
    near(0, 0)
    own(0, 2)
    gains(4, 5)
    own(0, 3)
    for j in range(1, narrow):
        swap(1, j).start()
    relay(0, 1)
    near(0, 1)
    far(0, 0)
    gains(6, 7)
    relay(0, 2)
    near(0, 2)
    relay(0, 3)
    near(0, 3)
    far(0, 1)
    relay(1, 0)
    near(1, 0)
    far(0, 2)
    far(0, 3)
    own(1, 1)
    settle(0)
    own(1, 2)
    table_loads[2].wait()
    for pair in range(depth // 2):
        lines(0, 2 * pair)
    own(1, 3)
    for s in range(slabs):
        cross_load(s).wait()

    events = (
        ((far, 0), (relay, 1), (near, 1)),
        ((relay, 2), (near, 2), (relay, 3), (near, 3)),
        ((far, 1), (far, 2), (far, 3)),
    )

    def steps(r, i):
        gather(2 * i + 1, slab_b)
        contract(r, 2 * i, slab_a)
        gather(lax.rem(2 * i + 2, slabs), slab_a)
        contract(r, 2 * i + 1, slab_b)

    def early(i, carry):
        steps(0, i)
        for at, batch in enumerate(events):

            @pl.when(i == at)
            def _():
                for event, j in batch:
                    event(1, j)

        return carry

    def late(i, carry):
        steps(1, 2 * i)
        steps(1, 2 * i + 1)
        return carry

    gather(0, slab_a)
    lax.fori_loop(0, slabs // 2, early, 0)
    settle(1)
    for pair in range(depth // 2):
        lines(1, 2 * pair)
    gather(0, slab_a)
    lax.fori_loop(0, slabs // 4, late, 0)

    for r in range(rounds):
        for j in range(narrow):
            if j > 0:
                swap(r, j).wait_send()
            for copy in own_copies(r, j):
                copy.wait_send()
            relay_copy(r, j).wait_send()
            for kind in range(1, 4):
                pass_copy(r, j, kind).wait_send()


def fused_device(image, deapodization, offsets, cross_weight, x_weight):
    wide = lax.axis_size("wide")
    narrow = lax.axis_size("narrow")
    block_x, block_y, width = image.shape[1:]
    depth = KZ // narrow
    slabs, samples, cells = cross_weight.shape[1:]
    rounds = 2
    strip = block_x // rounds
    lanes = 2 * block_y
    slots = 4
    z_table = complex_table(*base_tables(KZ, width, G, -(KZ // 2))).reshape(2 * KZ, 2 * width)
    cosine, sine = base_tables(G, width, G, -(G // 2))
    line_table = complex_table(cosine[: G // 2], sine[: G // 2]).reshape(G, 2, narrow, block_y // 2, 2)
    line_table = line_table.transpose(4, 0, 2, 1, 3)
    swapped = line_table[1].reshape(G, narrow // 2, 2, lanes // 2)[:, :, ::-1]
    line_table = np.stack([line_table[0].reshape(G, width), swapped.reshape(G, width)])
    row_table = np.stack([cosine, sine], axis=0).reshape(2, G, wide, rounds, strip)
    row_table = row_table.transpose(3, 0, 1, 2, 4).reshape(2 * rounds, G, wide * strip)
    hbm = pl.BlockSpec(memory_space=pl.ANY)
    vmem = pl.BlockSpec(memory_space=pltpu.VMEM)
    dma = pltpu.SemaphoreType.DMA
    half = wide * strip
    out = pl.pallas_call(
        functools.partial(fused_kernel, (depth, G, TILE if samples % TILE == 0 else samples)),
        out_shape=pltpu.VMEM((slabs, 2, samples), jnp.float32),
        in_specs=[hbm] * 8,
        out_specs=vmem,
        scratch_shapes=[
            pltpu.SMEM(deapodization.shape, jnp.float32),
            pltpu.VMEM(deapodization.shape, jnp.float32),
            pltpu.SMEM(offsets.shape, jnp.int32),
            pltpu.VMEM(image.shape, jnp.bfloat16),
            pltpu.VMEM((block_y, width), jnp.float32),
            pltpu.VMEM((width, width), jnp.bfloat16),
            pltpu.VMEM((KZ * (depth + 1), lanes), jnp.float32),
            pltpu.VMEM((rounds, narrow, depth, strip, lanes), jnp.bfloat16),
            pltpu.VMEM((rounds, narrow, wide, depth, strip, lanes), jnp.bfloat16),
            pltpu.VMEM(z_table.shape, jnp.bfloat16),
            pltpu.VMEM(line_table.shape, jnp.bfloat16),
            pltpu.VMEM(row_table.shape, jnp.bfloat16),
            pltpu.VMEM(row_table.shape, jnp.float32),
            pltpu.VMEM((slots, samples, BX), jnp.bfloat16),
            pltpu.VMEM((BX, 2 * width), jnp.bfloat16),
            pltpu.VMEM((BX, 2 * width), jnp.bfloat16),
            pltpu.VMEM((slabs, samples, 2 * width), jnp.bfloat16),
            pltpu.VMEM((slabs, samples, cells), jnp.bfloat16),
            pltpu.VMEM((2, G * (depth + 1), half), jnp.float32),
            pltpu.VMEM((cells, 2 * half), jnp.bfloat16),
            pltpu.VMEM((cells, 2 * half), jnp.bfloat16),
            dma((3,)),
            dma((rounds,)),
            dma((3,)),
            dma((slots,)),
            dma((slabs,)),
            dma((rounds, narrow)),
            dma((rounds, narrow)),
            dma((rounds, narrow, 2)),
            dma((rounds, narrow, 2)),
            dma((rounds, narrow)),
            dma((rounds, narrow)),
            dma((rounds, narrow, 4)),
            dma((rounds, narrow, 4)),
        ],
        compiler_params=pltpu.CompilerParams(
            vmem_limit_bytes=67043328 - 300 * 1024, collective_id=1, has_side_effects=True
        ),
    )(
        image, deapodization, offsets, jnp.asarray(z_table), jnp.asarray(line_table),
        jnp.asarray(row_table), x_weight[0], cross_weight[0],
    )
    return out[None]


def solution(mesh):
    square = mesh.shape["wide"] == 8 and mesh.shape["narrow"] == 4
    return jax.shard_map(
        fused_device if square else per_device,
        mesh=mesh,
        in_specs=(
            P(None, "wide", "narrow", None),
            P(),
            P(("wide", "narrow"), None),
            P(("wide", "narrow"), None, None, None),
            P(("wide", "narrow"), None, None, None),
        ),
        out_specs=P(("wide", "narrow"), None, None, None),
        check_vma=False,
    )
```

```python
import functools
import math

import jax
import jax.numpy as jnp
import numpy as np
from jax import lax
from jax.experimental import pallas as pl
from jax.experimental.pallas import tpu as pltpu
from jax.sharding import PartitionSpec as P

G = 512
KZ = 64
BX = 256
TILE = 128


def base_tables(out_rows, inputs, grid_size, lowest):
    frequency = np.arange(out_rows, dtype=np.int64) + lowest
    position = np.arange(inputs, dtype=np.int64) - inputs // 2
    phases = np.mod(frequency[:, None] * position[None, :], grid_size)
    angles = phases.astype(np.float64) * (2.0 * math.pi / grid_size)
    factor = 1.0 / math.sqrt(inputs)
    cosine = (np.cos(angles) * factor).astype(np.float32).astype(jnp.bfloat16)
    sine = (np.sin(angles) * factor).astype(np.float32).astype(jnp.bfloat16)
    return cosine, sine


def complex_table(cosine, sine):
    real_rows = np.stack([cosine, sine], axis=1)
    imag_rows = np.stack([-sine, cosine], axis=1)
    return np.stack([real_rows, imag_rows], axis=0)


def sample_kernel(
    sizes, offsets_ref, band_ref, line_ref, row_ref, x_ref, cross_ref, out_ref, wide_ref, slab_ref, window_ref
):
    depth, grid_rows, width, tile = sizes
    step = pl.program_id(0)
    cells = slab_ref.shape[0]

    @pl.when(step == 0)
    def _():
        def one_plane(k, carry):
            parts = [
                band_ref[:, piece, k].reshape(width, band_ref.shape[-1])
                for piece in range(band_ref.shape[1])
            ]
            plane = jnp.concatenate(parts, axis=-1) if len(parts) > 1 else parts[0]
            lines = lax.dot_general(
                line_ref[...], plane, (((1,), (1,)), ((), ())), preferred_element_type=jnp.float32
            )
            for part in range(2):
                for lane in range(0, width, 128):
                    wide_ref[(part * width + lane) // 128, pl.ds(k, grid_rows, stride=depth), :] = lines[
                        part * grid_rows : (part + 1) * grid_rows, lane : lane + 128
                    ]
            return carry

        for k in range(depth):
            one_plane(k, 0)

    here = pl.ds(pl.multiple_of(step * cells, cells), cells)
    start = offsets_ref[0, step]
    for block in range(2 * width // 128):
        lanes = slice(block * 128, (block + 1) * 128)
        slab_ref[:, lanes] = wide_ref[block, here, :].astype(jnp.bfloat16)
        window_ref[:, lanes] = row_ref[block, pl.ds(start, BX), :].astype(jnp.bfloat16)
    for first in range(0, cross_ref.shape[1], tile):
        rows = slice(first, first + tile)
        partial = jnp.dot(cross_ref[0, rows], slab_ref[...], preferred_element_type=jnp.float32)
        gain = jnp.dot(x_ref[0, rows], window_ref[...], preferred_element_type=jnp.float32)
        part_re, part_im = partial[:, :width], partial[:, width:]
        gain_cos, gain_sin = gain[:, :width], gain[:, width:]
        for part, value in enumerate(
            (gain_cos * part_re + gain_sin * part_im, gain_cos * part_im - gain_sin * part_re)
        ):
            folded = value[:, :128]
            for lane in range(128, width, 128):
                folded = folded + value[:, lane : lane + 128]
            out_ref[0, part : part + 1, rows] = jnp.sum(folded.T, axis=0, keepdims=True)


def gather_kernel(
    wide, narrow, band_ref, out_ref, own_sem, swap_send, swap_recv, chip_send, chip_recv, core_send, core_recv
):
    w = lax.axis_index("wide")
    n = lax.axis_index("narrow")
    sibling = w + 1 - 2 * lax.rem(w, 2)
    chips = wide // 2
    barrier = pltpu.get_barrier_semaphore()
    targets = [(w, lax.rem(n + j, narrow)) for j in range(1, narrow)]
    targets += [(lax.rem(w + 2 * j, wide), n) for j in range(1, chips)] + [(sibling, n)]
    for target in targets:
        pl.semaphore_signal(
            barrier, inc=1, device_id=target, device_id_type=pl.DeviceIdType.MESH
        )
    pl.semaphore_wait(barrier, len(targets))

    def remote(source, place, send, receive, target):
        return pltpu.make_async_remote_copy(
            src_ref=source,
            dst_ref=place,
            send_sem=send,
            recv_sem=receive,
            device_id=target,
            device_id_type=pl.DeviceIdType.MESH,
        )

    swaps = []
    for j in range(1, narrow):
        peer = lax.rem(n + j, narrow)
        swap = remote(
            band_ref.at[peer], out_ref.at[w, n], swap_send.at[j - 1], swap_recv.at[j - 1], (w, peer)
        )
        swap.start()
        swaps.append(swap)
    own = pltpu.make_async_copy(band_ref.at[n], out_ref.at[w, n], own_sem)
    own.start()
    own.wait()
    for swap in swaps:
        swap.wait()
    mine = out_ref.at[w]
    hops = []
    for j in range(1, chips):
        peer = lax.rem(w + 2 * j, wide)
        hop = remote(mine, mine, chip_send.at[j - 1], chip_recv.at[j - 1], (peer, n))
        hop.start()
        hops.append(hop)
    passes = [remote(mine, mine, core_send.at[0], core_recv.at[0], (sibling, n))]
    passes[0].start()
    for j in range(1, chips):
        hops[j - 1].wait_recv()
        block = out_ref.at[lax.rem(w + wide - 2 * j, wide)]
        forward = remote(block, block, core_send.at[j], core_recv.at[j], (sibling, n))
        forward.start()
        passes.append(forward)
    for hop in hops:
        hop.wait_send()
    for forward in passes:
        forward.wait()


def per_device(image, deapodization, offsets, cross_weight, x_weight):
    wide_count = lax.axis_size("wide")
    narrow_count = lax.axis_size("narrow")
    wide_index = lax.axis_index("wide")
    narrow_index = lax.axis_index("narrow")
    block_x = image.shape[1]
    block_y = image.shape[2]
    width = image.shape[3]
    depth = KZ // narrow_count
    samples, cells = cross_weight.shape[2], cross_weight.shape[3]
    scale_x = lax.dynamic_slice_in_dim(deapodization[0], wide_index * block_x, block_x)
    scale_y = lax.dynamic_slice_in_dim(deapodization[1], narrow_index * block_y, block_y)
    weighted = (
        image.astype(jnp.float32)
        * scale_x[None, :, None, None]
        * scale_y[None, None, :, None]
        * deapodization[2][None, None, None, :]
    ).astype(jnp.bfloat16)
    z_table = complex_table(*base_tables(KZ, width, G, -(KZ // 2)))
    band = jnp.einsum(
        "okcz,cxyz->kxoy", jnp.asarray(z_table), weighted, preferred_element_type=jnp.float32
    ).astype(jnp.bfloat16)
    band = band.reshape(KZ, block_x, 2 * block_y)
    band = band.reshape(narrow_count, depth, block_x, 2 * block_y)
    chips = wide_count // 2
    band = pl.pallas_call(
        functools.partial(gather_kernel, wide_count, narrow_count),
        out_shape=jax.ShapeDtypeStruct((wide_count,) + band.shape, band.dtype),
        in_specs=[pl.BlockSpec(memory_space=pltpu.VMEM)],
        out_specs=pl.BlockSpec(memory_space=pltpu.VMEM),
        scratch_shapes=[
            pltpu.SemaphoreType.DMA,
            pltpu.SemaphoreType.DMA((narrow_count - 1,)),
            pltpu.SemaphoreType.DMA((narrow_count - 1,)),
            pltpu.SemaphoreType.DMA((chips - 1,)),
            pltpu.SemaphoreType.DMA((chips - 1,)),
            pltpu.SemaphoreType.DMA((chips,)),
            pltpu.SemaphoreType.DMA((chips,)),
        ],
        compiler_params=pltpu.CompilerParams(collective_id=0, has_side_effects=True),
    )(band)
    if (2 * block_y) % 128:
        band = band.transpose(0, 2, 3, 1, 4).reshape(wide_count, 1, depth, block_x, 2 * width)

    cosine, sine = base_tables(G, width, G, -(G // 2))
    line_table = complex_table(cosine, sine).reshape(2 * G, 2, narrow_count, block_y)
    line_table = line_table.transpose(0, 2, 1, 3).reshape(2 * G, 2 * width)
    row_table = np.concatenate([cosine, sine], axis=1).astype(np.float32)
    row_table = row_table.reshape(G, 2 * width // 128, 128).transpose(1, 0, 2)

    tile = 512 if samples % 512 == 0 else samples
    kernel = functools.partial(sample_kernel, (depth, G, width, tile))
    out = pl.pallas_call(
        kernel,
        grid=(wide_count,),
        out_shape=jax.ShapeDtypeStruct((wide_count, 2, samples), jnp.float32),
        in_specs=[
            pl.BlockSpec(memory_space=pltpu.SMEM),
            pl.BlockSpec(band.shape, lambda s: (0, 0, 0, 0, 0)),
            pl.BlockSpec(line_table.shape, lambda s: (0, 0)),
            pl.BlockSpec(row_table.shape, lambda s: (0, 0, 0)),
            pl.BlockSpec((1, samples, BX), lambda s: (s, 0, 0)),
            pl.BlockSpec((1, samples, cells), lambda s: (s, 0, 0)),
        ],
        out_specs=pl.BlockSpec((1, 2, samples), lambda s: (s, 0, 0)),
        scratch_shapes=[
            pltpu.VMEM((2 * width // 128, G * depth, 128), jnp.float32),
            pltpu.VMEM((cells, 2 * width), jnp.bfloat16),
            pltpu.VMEM((BX, 2 * width), jnp.bfloat16),
        ],
        compiler_params=pltpu.CompilerParams(vmem_limit_bytes=60 * 1024 * 1024),
        cost_estimate=pl.CostEstimate(
            flops=2 * wide_count * samples * 2 * width * (cells + BX) + 8 * G * width * width * depth,
            bytes_accessed=2 * wide_count * samples * (cells + BX),
            transcendentals=0,
        ),
    )(offsets, band, jnp.asarray(line_table), jnp.asarray(row_table), x_weight[0], cross_weight[0])
    return out[None]


def flip(index, bits):
    low = lax.rem(index + bits, 2)
    high = lax.rem(lax.div(index, 2) + lax.div(bits, 2), 2)
    return low + 2 * high


def fused_kernel(
    sizes, image_hbm, deap_hbm, offsets_hbm, z_hbm, line_hbm, row_hbm, x_hbm, cross_hbm, out_ref,
    deap_smem, deap_ref, offsets_ref, image_ref, perm_ref, spread_ref, send_ref, grid_ref, z_ref, line_ref, packed_ref, row_ref, x_ref, window_a, window_b, gain_ref,
    cross_ref, wide_ref, slab_a, slab_b,
    small_sem, image_sem, table_sem, x_sem, cross_sem,
    swap_send, swap_recv, own_send, near_recv, relay_send, relay_recv, pass_send, pass_recv,
):
    depth, grid_rows, tile = sizes
    w = lax.axis_index("wide")
    n = lax.axis_index("narrow")
    rounds, narrow, wide, _, strip, lanes = grid_ref.shape
    windows = (window_a, window_b)
    slots = x_ref.shape[0]
    block_y, width = lanes // 2, perm_ref.shape[0]
    slabs, samples, cells = cross_ref.shape
    pitch = depth + 1
    half = wide * strip
    span = cells // depth

    core = lax.rem(w, 2)
    across = w + 2 - 4 * lax.rem(lax.div(w, 2), 2)
    along = w + 4 - 8 * lax.rem(lax.div(w, 4), 2)
    first = across + core * (along - across)
    second = along + core * (across - along)
    corner = across + along - w
    sibling = w + 1 - 2 * core
    held = (w, first, second, corner)
    straight = ((0, 3), (1, 3))
    sib_across = across + 1 - 2 * core
    sib_along = along + 1 - 2 * core
    sib_first = sib_along + core * (sib_across - sib_along)
    sib_second = sib_across + core * (sib_along - sib_across)
    theirs = (sibling, sib_first, sib_second, corner + 1 - 2 * core)

    def remote(source, place, send, receive, target):
        return pltpu.make_async_remote_copy(
            src_ref=source, dst_ref=place, send_sem=send, recv_sem=receive,
            device_id=target, device_id_type=pl.DeviceIdType.MESH,
        )

    image_loads = [
        pltpu.make_async_copy(
            image_hbm.at[:, r * strip : (r + 1) * strip],
            image_ref.at[:, r * strip : (r + 1) * strip],
            image_sem.at[r],
        )
        for r in range(rounds)
    ]
    table_loads = [
        pltpu.make_async_copy(source, place, table_sem.at[i])
        for i, (source, place) in enumerate(((z_hbm, z_ref), (row_hbm, packed_ref), (line_hbm, line_ref)))
    ]

    def x_load(s):
        return pltpu.make_async_copy(x_hbm.at[s], x_ref.at[s % slots], x_sem.at[s % slots])

    def cross_load(s):
        return pltpu.make_async_copy(cross_hbm.at[s], cross_ref.at[s], cross_sem.at[s])

    small_loads = [
        pltpu.make_async_copy(source, place, small_sem.at[i])
        for i, (source, place) in enumerate(((deap_hbm, deap_smem), (deap_hbm, deap_ref), (offsets_hbm, offsets_ref)))
    ]
    for copy in small_loads:
        copy.start()
    image_loads[0].start()
    table_loads[0].start()
    image_loads[1].start()
    barrier = pltpu.get_barrier_semaphore()
    peers = [(w, flip(n, j)) for j in range(1, narrow)] + [(first, n), (second, n), (corner, n), (sibling, n)]
    for peer in peers:
        pl.semaphore_signal(barrier, inc=1, device_id=peer, device_id_type=pl.DeviceIdType.MESH)

    row_at = lax.broadcasted_iota(jnp.int32, perm_ref.shape, 0)
    lane_at = lax.broadcasted_iota(jnp.int32, perm_ref.shape, 1)
    parity_at = lax.rem(lax.div(lax.rem(lane_at, lanes), block_y) + n, 2)
    line_at = lax.div(lax.rem(lane_at, block_y), block_y // 2)
    source_at = lax.div(lane_at, lanes) * lanes + line_at * block_y + 2 * lax.rem(lane_at, block_y // 2) + parity_at
    perm_ref[...] = jnp.where(row_at == source_at, 1.0, 0.0).astype(jnp.bfloat16)
    for copy in small_loads:
        copy.wait()
    last = deap_ref[2:3, :]
    lane = lax.broadcasted_iota(jnp.int32, (8, lanes), 1)
    middle = pltpu.roll(jnp.broadcast_to(deap_ref[1:2, :], (8, width)), width - n * block_y, 1)[:, :lanes]
    middle = jnp.where(lane < block_y, middle, pltpu.roll(middle, block_y, 1))

    def band(r):
        quarter = block_y // 2
        low = lax.rem(lax.broadcasted_iota(jnp.int32, (narrow * depth, lanes), 1), block_y) < quarter
        group = width // block_y
        rows = 2 * narrow * depth
        halves = []
        for c in range(2):
            pieces = []
            for x in range(strip):
                pieces.append((image_ref[c, r * strip + x].astype(jnp.float32) * last).astype(jnp.bfloat16))
            halves.append(jnp.concatenate(pieces, axis=0))
        both = jnp.concatenate(halves, axis=1)
        value = lax.dot_general(z_ref[...], both, (((1,), (1,)), ((), ())), preferred_element_type=jnp.float32)
        start = (w * rounds + r) * strip
        scales = [
            middle * jnp.where(lane < block_y, deap_smem[0, start + x], deap_smem[0, start + x + 1])
            for x in range(0, strip, 2)
        ]
        value = (value * jnp.concatenate(scales, axis=1)[:1]).astype(jnp.bfloat16)
        value = jnp.concatenate([value[:, at : at + width] for at in range(0, strip * block_y, width)], axis=0)
        value = jnp.dot(value, perm_ref[...], preferred_element_type=jnp.float32)
        for at in range(0, strip, group):
            real = value[at // group * rows : at // group * rows + rows // 2]
            imag = value[at // group * rows + rows // 2 : (at // group + 1) * rows]
            for pair in range(group // 2):
                here = slice(pair * lanes, (pair + 1) * lanes)
                even = jnp.where(low, real[:, here], pltpu.roll(imag[:, here], quarter, 1))
                odd = jnp.where(low, pltpu.roll(real[:, here], lanes - quarter, 1), imag[:, here])
                spread_ref[pl.ds(at + 2 * pair, narrow * depth, stride=pitch), :] = even
                spread_ref[pl.ds(at + 2 * pair + 1, narrow * depth, stride=pitch), :] = odd
        for k in range(narrow * depth):
            send_ref[r, k // depth, k % depth] = spread_ref[k * pitch : k * pitch + strip, :].astype(jnp.bfloat16)
        grid_ref[r, n, w] = send_ref[r, n]

    def swap(r, j):
        peer = flip(n, j)
        return remote(
            send_ref.at[r, peer], grid_ref.at[r, n, w], swap_send.at[r, j], swap_recv.at[r, j], (w, peer)
        )

    def place(r, j, column):
        return grid_ref.at[r, flip(n, j), column]

    def own_copies(r, j):
        mine = place(r, j, w)
        return [
            remote(mine, mine, own_send.at[r, j, 0], near_recv.at[r, j, 0], (first, n)),
            remote(mine, mine, own_send.at[r, j, 1], near_recv.at[r, j, 1], (second, n)),
            pass_copy(r, j, 0),
        ]

    def relay_copy(r, j):
        column, target = (w, corner) if (r, j) in straight else (first, second)
        block = place(r, j, column)
        return remote(block, block, relay_send.at[r, j], relay_recv.at[r, j], (target, n))

    def pass_copy(r, j, kind):
        block = place(r, j, held[kind])
        return remote(block, block, pass_send.at[r, j, kind], pass_recv.at[r, j, kind], (sibling, n))

    def arrived(r, j, column, send, receive):
        block = place(r, j, column)
        remote(block, block, send, receive, (sibling, n)).wait_recv()

    def own(r, j):
        if j > 0:
            block = grid_ref.at[r, flip(n, j), w]
            remote(block, block, swap_send.at[r, j], swap_recv.at[r, j], (w, flip(n, j))).wait_recv()
        for copy in own_copies(r, j):
            copy.start()
        if (r, j) in straight:
            relay_copy(r, j).start()

    def relay(r, j):
        arrived(r, j, first, own_send.at[r, j, 0], near_recv.at[r, j, 0])
        if (r, j) not in straight:
            relay_copy(r, j).start()
        pass_copy(r, j, 1).start()

    def near(r, j):
        arrived(r, j, second, own_send.at[r, j, 1], near_recv.at[r, j, 1])
        pass_copy(r, j, 2).start()

    def far(r, j):
        arrived(r, j, corner, relay_send.at[r, j], relay_recv.at[r, j])
        pass_copy(r, j, 3).start()

    def settle(r):
        for j in range(narrow):
            for kind in range(4):
                arrived(r, j, theirs[kind], pass_send.at[r, j, kind], pass_recv.at[r, j, kind])

    def gains(*batch):
        for s in batch:
            x_load(s).wait()
        for s, window in zip(batch, windows):
            start = offsets_ref[0, s]
            for block in range(row_ref.shape[0]):
                window[:, block * 128 : (block + 1) * 128] = row_ref[block, pl.ds(start, BX), :].astype(jnp.bfloat16)
            for at in range(0, samples, 512):
                rows = slice(at, at + 512)
                gain_ref[s, rows] = jnp.dot(
                    x_ref[s % slots, rows], window[...], preferred_element_type=jnp.float32
                ).astype(jnp.bfloat16)
        for s in batch:
            if s + slots < slabs:
                x_load(s + slots).start()
        for s in batch:
            cross_load(s).start()

    def lines(r, k):
        low = lax.broadcasted_iota(jnp.int32, (2 * half, lanes), 1) < block_y
        planes = [
            jnp.concatenate([grid_ref[r, source, :, k + i].reshape(half, lanes) for i in range(2)], axis=0)
            for source in range(narrow)
        ]
        evens, odds = [], []
        for one, two in zip(planes[::2], planes[1::2]):
            evens.append(jnp.where(low, one, two))
            odds.append(jnp.where(low, two, one))
        even, odd = [
            lax.dot_general(
                line_ref[parity], jnp.concatenate(pieces, axis=1), (((1,), (1,)), ((), ())),
                preferred_element_type=jnp.float32,
            )
            for parity, pieces in enumerate((evens, odds))
        ]
        for sign, value in enumerate((even + odd, even - odd)):
            for part in range(2):
                for i in range(2):
                    wide_ref[part, pl.ds(sign * (grid_rows // 2) * pitch + k + i, grid_rows // 2, stride=pitch), :] = value[
                        part * grid_rows // 2 : (part + 1) * grid_rows // 2, i * half : (i + 1) * half
                    ]

    def gather(s, slab_ref):
        base = s * span * pitch
        for part in range(2):
            for y in range(span):
                slab_ref[y * depth : (y + 1) * depth, part * half : (part + 1) * half] = wide_ref[
                    part, pl.ds(base + y * pitch, depth), :
                ].astype(jnp.bfloat16)

    def contract(r, s, slab_ref):
        for at in range(0, samples, tile):
            rows = slice(at, at + tile)
            value = jnp.dot(cross_ref[s, rows], slab_ref[...], preferred_element_type=jnp.float32)
            real, imag = value[:, :half], value[:, half:]
            gain = gain_ref[s, rows, 2 * r * half : 2 * (r + 1) * half].astype(jnp.float32)
            cosine, sine = gain[:, :half], gain[:, half:]
            for part, product in enumerate((cosine * real + sine * imag, cosine * imag - sine * real)):
                total = jnp.sum(product.T, axis=0, keepdims=True)
                if r > 0:
                    total = total + out_ref[s, part : part + 1, rows]
                out_ref[s, part : part + 1, rows] = total

    for copy in table_loads[1:]:
        copy.start()
    for s in range(slots):
        x_load(s).start()
    table_loads[0].wait()
    image_loads[0].wait()
    band(0)
    pl.semaphore_wait(barrier, len(peers))
    for j in range(1, narrow):
        swap(0, j).start()
    own(0, 0)
    image_loads[1].wait()
    band(1)
    own(1, 0)
    table_loads[1].wait()
    row_ref[...] = packed_ref[...].astype(jnp.float32)
    gains(0, 1)
    gains(2, 3)
    relay(0, 0)
    own(0, 1)
    near(0, 0)
    gains(4, 5)
    own(0, 2)
    gains(6, 7)
    own(0, 3)
    for j in range(1, narrow):
        swap(1, j).start()
    relay(0, 1)
    far(0, 0)
    near(0, 1)
    relay(0, 2)
    near(0, 2)
    relay(0, 3)
    near(0, 3)
    far(0, 1)
    relay(1, 0)
    near(1, 0)
    far(0, 2)
    far(0, 3)
    own(1, 1)
    settle(0)
    own(1, 2)
    table_loads[2].wait()
    for pair in range(depth // 2):
        lines(0, 2 * pair)
    own(1, 3)
    for s in range(slabs):
        cross_load(s).wait()

    events = (
        ((far, 0), (relay, 1), (near, 1), (relay, 2), (near, 2), (relay, 3), (near, 3)),
        ((far, 1), (far, 2), (far, 3)),
    )

    def steps(r, i):
        gather(2 * i + 1, slab_b)
        contract(r, 2 * i, slab_a)
        gather(lax.rem(2 * i + 2, slabs), slab_a)
        contract(r, 2 * i + 1, slab_b)

    def early(i, carry):
        steps(0, 2 * i)
        steps(0, 2 * i + 1)
        for at, batch in enumerate(events):

            @pl.when(i == at)
            def _():
                for event, j in batch:
                    event(1, j)

        return carry

    def late(i, carry):
        steps(1, 2 * i)
        steps(1, 2 * i + 1)
        return carry

    gather(0, slab_a)
    lax.fori_loop(0, slabs // 4, early, 0)
    settle(1)
    for pair in range(depth // 2):
        lines(1, 2 * pair)
    gather(0, slab_a)
    lax.fori_loop(0, slabs // 4, late, 0)

    for r in range(rounds):
        for j in range(narrow):
            if j > 0:
                swap(r, j).wait_send()
            for copy in own_copies(r, j):
                copy.wait_send()
            relay_copy(r, j).wait_send()
            for kind in range(1, 4):
                pass_copy(r, j, kind).wait_send()


def fused_device(image, deapodization, offsets, cross_weight, x_weight):
    wide = lax.axis_size("wide")
    narrow = lax.axis_size("narrow")
    block_x, block_y, width = image.shape[1:]
    depth = KZ // narrow
    slabs, samples, cells = cross_weight.shape[1:]
    rounds = 2
    strip = block_x // rounds
    lanes = 2 * block_y
    slots = slabs
    z_table = complex_table(*base_tables(KZ, width, G, -(KZ // 2))).reshape(2 * KZ, 2 * width)
    cosine, sine = base_tables(G, width, G, -(G // 2))
    line_table = complex_table(cosine[: G // 2], sine[: G // 2]).reshape(G, 2, narrow, block_y // 2, 2)
    line_table = line_table.transpose(4, 0, 2, 1, 3)
    swapped = line_table[1].reshape(G, narrow // 2, 2, lanes // 2)[:, :, ::-1]
    line_table = np.stack([line_table[0].reshape(G, width), swapped.reshape(G, width)])
    row_table = np.stack([cosine, sine], axis=0).reshape(2, G, wide, rounds, strip)
    row_table = row_table.transpose(3, 0, 1, 2, 4).reshape(2 * rounds, G, wide * strip)
    hbm = pl.BlockSpec(memory_space=pl.ANY)
    vmem = pl.BlockSpec(memory_space=pltpu.VMEM)
    dma = pltpu.SemaphoreType.DMA
    half = wide * strip
    out = pl.pallas_call(
        functools.partial(fused_kernel, (depth, G, TILE if samples % TILE == 0 else samples)),
        out_shape=pltpu.VMEM((slabs, 2, samples), jnp.float32),
        in_specs=[hbm] * 8,
        out_specs=vmem,
        scratch_shapes=[
            pltpu.SMEM(deapodization.shape, jnp.float32),
            pltpu.VMEM(deapodization.shape, jnp.float32),
            pltpu.SMEM(offsets.shape, jnp.int32),
            pltpu.VMEM(image.shape, jnp.bfloat16),
            pltpu.VMEM((width, width), jnp.bfloat16),
            pltpu.VMEM((KZ * (depth + 1), lanes), jnp.float32),
            pltpu.VMEM((rounds, narrow, depth, strip, lanes), jnp.bfloat16),
            pltpu.VMEM((rounds, narrow, wide, depth, strip, lanes), jnp.bfloat16),
            pltpu.VMEM(z_table.shape, jnp.bfloat16),
            pltpu.VMEM(line_table.shape, jnp.bfloat16),
            pltpu.VMEM(row_table.shape, jnp.bfloat16),
            pltpu.VMEM(row_table.shape, jnp.float32),
            pltpu.VMEM((slots, samples, BX), jnp.bfloat16),
            pltpu.VMEM((BX, 2 * width), jnp.bfloat16),
            pltpu.VMEM((BX, 2 * width), jnp.bfloat16),
            pltpu.VMEM((slabs, samples, 2 * width), jnp.bfloat16),
            pltpu.VMEM((slabs, samples, cells), jnp.bfloat16),
            pltpu.VMEM((2, G * (depth + 1), half), jnp.float32),
            pltpu.VMEM((cells, 2 * half), jnp.bfloat16),
            pltpu.VMEM((cells, 2 * half), jnp.bfloat16),
            dma((3,)),
            dma((rounds,)),
            dma((3,)),
            dma((slots,)),
            dma((slabs,)),
            dma((rounds, narrow)),
            dma((rounds, narrow)),
            dma((rounds, narrow, 2)),
            dma((rounds, narrow, 2)),
            dma((rounds, narrow)),
            dma((rounds, narrow)),
            dma((rounds, narrow, 4)),
            dma((rounds, narrow, 4)),
        ],
        compiler_params=pltpu.CompilerParams(
            vmem_limit_bytes=67043328 - 300 * 1024, collective_id=1, has_side_effects=True
        ),
    )(
        image, deapodization, offsets, jnp.asarray(z_table), jnp.asarray(line_table),
        jnp.asarray(row_table), x_weight[0], cross_weight[0],
    )
    return out[None]


def solution(mesh):
    square = mesh.shape["wide"] == 8 and mesh.shape["narrow"] == 4
    return jax.shard_map(
        fused_device if square else per_device,
        mesh=mesh,
        in_specs=(
            P(None, "wide", "narrow", None),
            P(),
            P(("wide", "narrow"), None),
            P(("wide", "narrow"), None, None, None),
            P(("wide", "narrow"), None, None, None),
        ),
        out_specs=P(("wide", "narrow"), None, None, None),
        check_vma=False,
    )
```
